128 devices in a mesh: mem: 4 (over x_lo, core), slab: 32 (over z, y, x_hi).
Axes of the slice: x: 4 (x_hi: 2, x_lo: 2; x = x_hi * 2 + x_lo), y: 4, z: 4, core: 2. Of those that a mesh axis runs over, the one named last changes fastest.
Arguments:
- anomalies: bfloat16 [8, 4096, 4096], P('mem', 'slab'), may hold values from -2.390625 to 2.390625
- increment: float32 [4096, 4096], P('slab'), may hold values from -6 to 6
- spectrum: float32 [4096, 4096], P(None, 'slab'), may hold values from 0.01 to 2, as said below
Outputs:
- product: float32 [4096, 4096], P('slab')
The draws below stay inside these ranges and needn't reach their ends.
Inputs may be any that keep to these rules, and one draw needn't show every extreme that they name: spectrum[k, l] equals spectrum[(4096 - k) % 4096, (4096 - l) % 4096], and is positive.
All inputs are finite; a program needn't handle non-finite values.
Results may differ from the reference program's by a relative error of at most 0.0003.
Values sent between devices are 32-bit elements; how exact they have to be, the bound alone decides.
A program may use at most 128 MiB of HBM per device.

```python
import jax
import jax.numpy as jnp
from jax import lax

NX = 4096
NY = 4096
MEMBERS = 8


def draw_spectrum(key, part):
    logs = jax.random.uniform(key, (NX, NY), jnp.float32, jnp.log(0.05), 0.0)
    values = jnp.exp(logs)
    mirrored = jnp.roll(jnp.flip(values, (0, 1)), 1, (0, 1))
    result = 0.5 * (values + mirrored)
    return result


def shard_levels(own_key, extent, split, low, top_value):
    loudness, own = 1.0, jax.random.fold_in(own_key, 6)
    for dim, shards_of in split:
        steps = jnp.exp(jax.random.uniform(jax.random.fold_in(own, dim), (shards_of,), jnp.float32, low / len(split), top_value / len(split)))
        loudness = loudness * jnp.repeat(steps, extent[dim] // shards_of).reshape([-1 if axis == dim else 1 for axis in range(len(extent))])
    return loudness


def noise(key, shape, spread, limit, pieces=(), held_as=jnp.bfloat16):
    level = shard_levels(key, shape, pieces, -0.22, 0.18) if pieces else 1.0
    array = jax.random.normal(key, shape, jnp.float32) * spread * level
    return jnp.minimum(jnp.maximum(array, -limit), limit).astype(held_as)


def setup_inputs(seed: int = 0) -> dict:
    streams_of = jax.random.split(jax.random.key(seed), 4)
    anomalies = noise(streams_of[0], (MEMBERS, NX, NY), 0.4, 2.390625, ((0, 4), (1, 32)))
    increment = noise(streams_of[1], (NX, NY), 1.0, 6.0, ((0, 32),), jnp.float32)
    spectrum = draw_spectrum(jax.random.fold_in(streams_of[3], 71), 0)
    return {"anomalies": anomalies, "increment": increment, "spectrum": spectrum}


def reference(anomalies, increment, spectrum):
    def member_term(index, total):
        member = lax.dynamic_index_in_dim(anomalies, index, 0, keepdims=False).astype(jnp.float32)
        field = member * increment
        waves = jnp.fft.fft2(field)
        filtered = jnp.real(jnp.fft.ifft2(waves * spectrum))
        return total + member * filtered

    start = jnp.zeros((NX, NY), jnp.float32)
    return lax.fori_loop(0, MEMBERS, member_term, start)
```

```python
import math

import jax
import jax.numpy as jnp
import numpy as np
from jax import lax
from jax.experimental import pallas as pl
from jax.experimental.pallas import tpu as pltpu
from jax.sharding import PartitionSpec as P

MESH = pl.DeviceIdType.MESH
F32 = jnp.float32
BF16 = jnp.bfloat16
ROOT_HALF = math.sqrt(0.5)

ROUNDS = (
    (2, 2), (1, 1), (3, 3), (0, 0), (1, 3), (3, 1), (0, 2), (2, 0),
    (1, 0), (3, 2), (1, 2), (3, 0), (0, 1), (2, 3), (2, 1), (0, 3),
)
OFFSETS = tuple(
    offset
    for a, b in ROUNDS
    for offset in ((a, b, 1), ((a + 2) % 4, (b + 2) % 4, 0))
    if offset != (0, 0, 0)
)


def constant_tables():
    index = np.arange(128)
    angle = 2.0 * np.pi / 128 * (np.outer(index, index) % 128)
    cos, sin = np.cos(angle), np.sin(angle)
    tables = []
    for sign in (-1.0, 1.0):
        block = np.block([[cos, sign * sin], [-sign * sin, cos]])
        if sign < 0:
            flipped = block.T
            high = flipped.astype(BF16)
            low = (flipped - high.astype(np.float64)).astype(BF16)
            tables.append(np.concatenate([high, high, low], axis=1))
        high = block.astype(BF16)
        low = (block - high.astype(np.float64)).astype(BF16)
        tables.append(np.concatenate([high, high, low], axis=0))
    twist = 2.0 * np.pi / 4096 * np.outer(np.arange(32), index)
    twist = np.stack([np.cos(twist), np.sin(twist)]).astype(np.float32)
    twist = np.broadcast_to(twist[:, :, None, :], (2, 32, 8, 128)).copy()
    return tables, twist


def short_transform(values, sign):
    count = len(values)
    if count == 1:
        return values
    even = short_transform(values[0::2], sign)
    odd = short_transform(values[1::2], sign)
    first, second = [], []
    for k in range(count // 2):
        (er, ei), (xr, xi) = even[k], odd[k]
        if k == 0:
            tr, ti = xr, xi
        elif 4 * k == count:
            if sign > 0:
                first.append((er - xi, ei + xr))
                second.append((er + xi, ei - xr))
            else:
                first.append((er + xi, ei - xr))
                second.append((er - xi, ei + xr))
            continue
        elif 8 * k == count:
            tr = (xr - sign * xi if sign > 0 else xr + xi) * ROOT_HALF
            ti = (xi + xr if sign > 0 else xi - xr) * ROOT_HALF
        elif 8 * k == 3 * count:
            tr = (xr + xi if sign > 0 else xr - xi) * -ROOT_HALF
            ti = (xr - xi if sign > 0 else -xr - xi) * ROOT_HALF
        else:
            cos = math.cos(2.0 * math.pi * k / count)
            sin = sign * math.sin(2.0 * math.pi * k / count)
            tr = xr * cos - xi * sin
            ti = xr * sin + xi * cos
        first.append((er + tr, ei + ti))
        second.append((er - tr, ei - ti))
    return first + second


def three_parts(x):
    high = x.astype(BF16)
    low = (x - high.astype(F32)).astype(BF16)
    return jnp.concatenate([high, low, high], axis=1)


def kernel(
    anomalies, increment, spectrum, forward_flip, forward, inverse, twist, out,
    anom, incr, spec, spec_flip, field_re, field_im, work, send_a, recv_a,
    column, send_b, recv_b, part, recv_part, pair, recv_pair, total,
    load_sem, send_a_sem, recv_a_sem, send_b_sem, recv_b_sem, part_sems, pair_sems, total_sems,
    out_sem,
):
    me = lax.axis_index("slab")
    mem = lax.axis_index("mem")
    z, y, x = me // 8, (me // 2) % 4, me % 2
    core = mem % 2
    other_core = (mem // 2) * 2 + (1 - core)
    other_chip = (1 - mem // 2) * 2 + core

    def slab_at(offset):
        dz, dy, dx = offset
        return ((z + dz) % 4) * 8 + ((y + dy) % 4) * 2 + (x + dx) % 2

    loads = [
        pltpu.make_async_copy(anomalies, anom, load_sem.at[0]),
        pltpu.make_async_copy(increment, incr, load_sem.at[1]),
        pltpu.make_async_copy(spectrum, spec, load_sem.at[2]),
    ]
    for copy in loads:
        copy.start()

    barrier = pltpu.get_barrier_semaphore()
    for offset in OFFSETS:
        pl.semaphore_signal(
            barrier, inc=1, device_id={"mem": mem, "slab": slab_at(offset)}, device_id_type=MESH
        )
    for mate in (other_core, other_chip):
        pl.semaphore_signal(
            barrier, inc=1, device_id={"mem": mate, "slab": me}, device_id_type=MESH
        )

    sub = lax.broadcasted_iota(jnp.int32, (16, 8, 128), 1)
    lower = sub < 4

    def interlaced(a, b):
        even = jnp.where(lower, a, pltpu.roll(b, 4, 1))
        odd = jnp.where(lower, pltpu.roll(a, 4, 1), b)
        return even, odd

    def twisted(values, sign):
        result = [values[0]]
        for k in range(1, 32):
            re, im = values[k]
            cos, sin = twist[0, k], twist[1, k]
            if sign > 0:
                result.append((re * cos - im * sin, re * sin + im * cos))
            else:
                result.append((re * cos + im * sin, im * cos - re * sin))
        return result

    loads[0].wait()
    loads[1].wait()

    def multiply(b, carry):
        rows = pl.ds(pl.multiple_of(b * 16, 16), 16)
        step = incr[rows, :]
        field_re[rows, :] = anom[0, rows, :].astype(F32) * step
        field_im[rows, :] = anom[1, rows, :].astype(F32) * step
        return carry

    lax.fori_loop(0, 8, multiply, 0)

    def forward_rows(g, carry):
        rows = pl.ds(pl.multiple_of(g * 8, 8), 8)
        values = [
            (field_re[rows, 128 * a : 128 * a + 128], field_im[rows, 128 * a : 128 * a + 128])
            for a in range(32)
        ]
        values = twisted(short_transform(values, -1), -1)
        for a in range(32):
            work[a, rows, 0:128] = values[a][0]
            work[a, rows, 128:256] = values[a][1]
        return carry

    lax.fori_loop(0, 16, forward_rows, 0)

    pl.semaphore_wait(barrier, len(OFFSETS) + 2)

    def send_copy(source, target, send_sem, recv_sem, chunk, slab):
        return pltpu.make_async_remote_copy(
            src_ref=source.at[chunk, slab],
            dst_ref=target.at[chunk, me],
            send_sem=send_sem.at[chunk],
            recv_sem=recv_sem.at[chunk],
            device_id={"mem": mem, "slab": slab},
            device_id_type=MESH,
        )

    def whole_copy(source, target, send_sem, recv_sem, chunk):
        return pltpu.make_async_remote_copy(
            src_ref=source.at[chunk, 0:31],
            dst_ref=target.at[chunk, 0:31],
            send_sem=send_sem.at[chunk],
            recv_sem=recv_sem.at[chunk],
            device_id={"mem": other_core, "slab": me},
            device_id_type=MESH,
        )

    def forward_send(chunk, carry):
        def one_pair(p, inner):
            first = pl.multiple_of(chunk * 8 + p * 2, 2)
            both = three_parts(work[pl.ds(first, 2)].reshape(256, 256))
            result = lax.dot_general(
                forward_flip[...], both, (((1,), (1,)), ((), ())), preferred_element_type=F32
            )
            rows = pl.ds(pl.multiple_of(p * 8, 8), 8)
            for part_at in range(2):
                piece = result[128 * part_at : 128 * part_at + 128]
                even, odd = interlaced(
                    piece[:, :128].reshape(16, 8, 128), piece[:, 128:].reshape(16, 8, 128)
                )
                for d in range(16):
                    send_a[chunk, 2 * d, part_at, rows, :] = even[d]
                    send_a[chunk, 2 * d + 1, part_at, rows, :] = odd[d]
            return inner

        lax.fori_loop(0, 4, one_pair, 0)
        for offset in OFFSETS:
            send_copy(send_a, recv_a, send_a_sem, recv_a_sem, chunk, slab_at(offset)).start()
        recv_a[chunk, me] = send_a[chunk, me]
        return carry

    lax.fori_loop(0, 4, forward_send, 0)

    loads[2].wait()

    def flip_spectrum(k, carry):
        piece = spec[pl.ds(k, 128, stride=32), :] * (1.0 / (4096.0 * 4096.0))
        piece = piece.T
        for b in range(4):
            spec_flip[k, pl.ds(b, 32, stride=4), :] = piece[32 * b : 32 * b + 32]
        return carry

    lax.fori_loop(0, 32, flip_spectrum, 0)

    def columns(chunk, carry):
        whole_copy(send_a, recv_a, send_a_sem, recv_a_sem, chunk).wait_recv()

        def down(q, inner):
            rows = pl.ds(pl.multiple_of(q * 8, 8), 8)
            values = [
                (recv_a[chunk, s, 0, rows, :], recv_a[chunk, s, 1, rows, :]) for s in range(32)
            ]
            values = twisted(short_transform(values, -1), -1)
            for k in range(32):
                column[k, rows, 0:128] = values[k][0]
                column[k, rows, 128:256] = values[k][1]
            return inner

        lax.fori_loop(0, 4, down, 0)
        share = pl.ds(pl.multiple_of(chunk * 32, 32), 32)

        def across(g, inner):
            group = pl.ds(pl.multiple_of(g * 8, 8), 8)
            waves = jnp.dot(
                three_parts(column[group].reshape(256, 256)), forward[...],
                preferred_element_type=F32,
            )
            scale = spec_flip[group, share, :].reshape(256, 128)
            waves = jnp.concatenate([waves[:, :128] * scale, waves[:, 128:] * scale], axis=1)
            back = jnp.dot(three_parts(waves), inverse[...], preferred_element_type=F32)
            column[group] = back.reshape(8, 32, 256)
            return inner

        lax.fori_loop(0, 4, across, 0)

        def up(q, inner):
            rows = pl.ds(pl.multiple_of(q * 8, 8), 8)
            values = [(column[k, rows, 0:128], column[k, rows, 128:256]) for k in range(32)]
            values = short_transform(twisted(values, 1), 1)
            for s in range(32):
                send_b[chunk, s, 0, rows, :] = values[s][0]
                send_b[chunk, s, 1, rows, :] = values[s][1]
            return inner

        lax.fori_loop(0, 4, up, 0)
        for offset in OFFSETS:
            send_copy(send_b, recv_b, send_b_sem, recv_b_sem, chunk, slab_at(offset)).start()
        recv_b[chunk, me] = send_b[chunk, me]
        return carry

    lax.fori_loop(0, 4, columns, 0)

    def inverse_rows(chunk, carry):
        whole_copy(send_b, recv_b, send_b_sem, recv_b_sem, chunk).wait_recv()

        def one_pair(p, inner):
            rows = pl.ds(pl.multiple_of(p * 8, 8), 8)
            halves = []
            for part_at in range(2):
                even = jnp.stack([recv_b[chunk, 2 * d, part_at, rows, :] for d in range(16)])
                odd = jnp.stack([recv_b[chunk, 2 * d + 1, part_at, rows, :] for d in range(16)])
                a, b = interlaced(even, odd)
                halves.append((a.reshape(128, 128).T, b.reshape(128, 128).T))
            both = jnp.concatenate(
                [
                    jnp.concatenate([halves[0][i], halves[1][i]], axis=1)
                    for i in range(2)
                ],
                axis=0,
            )
            result = jnp.dot(three_parts(both), inverse[...], preferred_element_type=F32)
            for i in range(2):
                at = chunk * 8 + p * 2 + i
                cos, sin = twist[0, at, 0:1, :], twist[1, at, 0:1, :]
                re = result[128 * i : 128 * i + 128, :128]
                im = result[128 * i : 128 * i + 128, 128:]
                work[at, :, 0:128] = re * cos - im * sin
                work[at, :, 128:256] = re * sin + im * cos
            return inner

        lax.fori_loop(0, 4, one_pair, 0)
        return carry

    lax.fori_loop(0, 4, inverse_rows, 0)

    def member_sum(b):
        for half in range(2):
            rows = pl.ds(pl.multiple_of(b * 16 + half * 8, 8), 8)
            values = [(work[a, rows, 0:128], work[a, rows, 128:256]) for a in range(32)]
            values = short_transform(values, 1)
            for a in range(32):
                field_re[rows, 128 * a : 128 * a + 128] = values[a][0]
                field_im[rows, 128 * a : 128 * a + 128] = values[a][1]
        rows = pl.ds(pl.multiple_of(b * 16, 16), 16)
        part[b] = (
            anom[0, rows, :].astype(F32) * field_re[rows, :]
            + anom[1, rows, :].astype(F32) * field_im[rows, :]
        )

    def to_core(t):
        return pltpu.make_async_remote_copy(
            src_ref=part.at[2 * t + 1 - core],
            dst_ref=recv_part.at[t],
            send_sem=part_sems.at[0, t],
            recv_sem=part_sems.at[1, t],
            device_id={"mem": other_core, "slab": me},
            device_id_type=MESH,
        )

    def to_chip(t):
        return pltpu.make_async_remote_copy(
            src_ref=pair.at[t],
            dst_ref=recv_pair.at[t],
            send_sem=pair_sems.at[0, t],
            recv_sem=pair_sems.at[1, t],
            device_id={"mem": other_chip, "slab": me},
            device_id_type=MESH,
        )

    def finished(t):
        return pltpu.make_async_remote_copy(
            src_ref=total.at[2 * t + core],
            dst_ref=total.at[2 * t + core],
            send_sem=total_sems.at[0, t],
            recv_sem=total_sems.at[1, t],
            device_id={"mem": other_core, "slab": me},
            device_id_type=MESH,
        )

    def write_out(block):
        return pltpu.make_async_copy(
            total.at[block],
            out.at[pl.ds(pl.multiple_of(block * 16, 16), 16), :],
            out_sem.at[block],
        )

    def sum_and_send(t, carry):
        member_sum(2 * t + 1 - core)
        to_core(t).start()
        member_sum(2 * t + core)
        to_core(t).wait_recv()
        pair[t] = part[2 * t + core] + recv_part[t]
        to_chip(t).start()
        return carry

    lax.fori_loop(0, 4, sum_and_send, 0)

    def finish(t, carry):
        to_chip(t).wait_recv()
        total[2 * t + core] = pair[t] + recv_pair[t]
        finished(t).start()
        write_out(2 * t + core).start()
        return carry

    lax.fori_loop(0, 4, finish, 0)

    def collect(t, carry):
        finished(t).wait_recv()
        write_out(2 * t + 1 - core).start()
        return carry

    lax.fori_loop(0, 4, collect, 0)

    def drain(t, carry):
        whole_copy(send_a, recv_a, send_a_sem, recv_a_sem, t).wait_send()
        whole_copy(send_b, recv_b, send_b_sem, recv_b_sem, t).wait_send()
        to_core(t).wait_send()
        to_chip(t).wait_send()
        finished(t).wait_send()
        write_out(2 * t).wait()
        write_out(2 * t + 1).wait()
        return carry

    lax.fori_loop(0, 4, drain, 0)


def per_device(anomalies, increment, spectrum):
    tables, twist = constant_tables()
    vmem = pl.BlockSpec(memory_space=pltpu.VMEM)
    anywhere = pl.BlockSpec(memory_space=pl.ANY)
    dma = pltpu.SemaphoreType.DMA
    return pl.pallas_call(
        kernel,
        out_shape=jax.ShapeDtypeStruct((128, 4096), F32),
        in_specs=[anywhere] * 3 + [vmem] * 4,
        out_specs=anywhere,
        scratch_shapes=[
            pltpu.VMEM((2, 128, 4096), BF16),
            pltpu.VMEM((128, 4096), F32),
            pltpu.VMEM((4096, 128), F32),
            pltpu.VMEM((32, 128, 128), F32),
            pltpu.VMEM((128, 4096), F32),
            pltpu.VMEM((128, 4096), F32),
            pltpu.VMEM((32, 128, 256), F32),
            pltpu.VMEM((4, 32, 2, 32, 128), F32),
            pltpu.VMEM((4, 32, 2, 32, 128), F32),
            pltpu.VMEM((32, 32, 256), F32),
            pltpu.VMEM((4, 32, 2, 32, 128), F32),
            pltpu.VMEM((4, 32, 2, 32, 128), F32),
            pltpu.VMEM((8, 16, 4096), F32),
            pltpu.VMEM((4, 16, 4096), F32),
            pltpu.VMEM((4, 16, 4096), F32),
            pltpu.VMEM((4, 16, 4096), F32),
            pltpu.VMEM((8, 16, 4096), F32),
            dma((3,)),
            dma((4,)), dma((4,)), dma((4,)), dma((4,)),
            dma((2, 4)), dma((2, 4)), dma((2, 4)),
            dma((8,)),
        ],
        compiler_params=pltpu.CompilerParams(
            collective_id=0, has_side_effects=True, vmem_limit_bytes=67043328
        ),
        name="covariance",
    )(anomalies, increment, spectrum, *[jnp.asarray(t) for t in tables], jnp.asarray(twist))


def solution(mesh):
    placed = (P("mem", "slab", None), P("slab", None), P(None, "slab"))
    return jax.shard_map(
        per_device, mesh=mesh, in_specs=placed, out_specs=P("slab", None), check_vma=False
    )
```

```python
import math

import jax
import jax.numpy as jnp
import numpy as np
from jax import lax
from jax.experimental import pallas as pl
from jax.experimental.pallas import tpu as pltpu
from jax.sharding import PartitionSpec as P

MESH = pl.DeviceIdType.MESH
F32 = jnp.float32
BF16 = jnp.bfloat16
ROOT_HALF = math.sqrt(0.5)

ROUNDS = (
    (2, 2), (1, 1), (3, 3), (0, 0), (1, 3), (3, 1), (0, 2), (2, 0),
    (1, 0), (3, 2), (1, 2), (3, 0), (0, 1), (2, 3), (2, 1), (0, 3),
)
OFFSETS = tuple(
    offset
    for a, b in ROUNDS
    for offset in ((a, b, 1), ((a + 2) % 4, (b + 2) % 4, 0))
    if offset != (0, 0, 0)
)


def constant_tables():
    index = np.arange(128)
    angle = 2.0 * np.pi / 128 * (np.outer(index, index) % 128)
    cos, sin = np.cos(angle), np.sin(angle)
    tables = []
    for sign in (-1.0, 1.0):
        block = np.block([[cos, sign * sin], [-sign * sin, cos]])
        if sign < 0:
            flipped = block.T
            high = flipped.astype(BF16)
            low = (flipped - high.astype(np.float64)).astype(BF16)
            tables.append(np.concatenate([high, high, low], axis=1))
        high = block.astype(BF16)
        low = (block - high.astype(np.float64)).astype(BF16)
        tables.append(np.concatenate([high, high, low], axis=0))
    order = np.arange(32) % 8 * 4 + np.arange(32) // 8
    twist = 2.0 * np.pi / 4096 * np.outer(order, index)
    twist = np.stack([np.cos(twist), np.sin(twist)]).astype(np.float32)
    twist = np.broadcast_to(twist[:, :, None, :], (2, 32, 8, 128)).copy()
    return tables, twist


def short_transform(values, sign):
    count = len(values)
    if count == 1:
        return values
    even = short_transform(values[0::2], sign)
    odd = short_transform(values[1::2], sign)
    first, second = [], []
    for k in range(count // 2):
        (er, ei), (xr, xi) = even[k], odd[k]
        if k == 0:
            tr, ti = xr, xi
        elif 4 * k == count:
            if sign > 0:
                first.append((er - xi, ei + xr))
                second.append((er + xi, ei - xr))
            else:
                first.append((er + xi, ei - xr))
                second.append((er - xi, ei + xr))
            continue
        elif 8 * k == count:
            tr = (xr - sign * xi if sign > 0 else xr + xi) * ROOT_HALF
            ti = (xi + xr if sign > 0 else xi - xr) * ROOT_HALF
        elif 8 * k == 3 * count:
            tr = (xr + xi if sign > 0 else xr - xi) * -ROOT_HALF
            ti = (xr - xi if sign > 0 else -xr - xi) * ROOT_HALF
        else:
            cos = math.cos(2.0 * math.pi * k / count)
            sin = sign * math.sin(2.0 * math.pi * k / count)
            tr = xr * cos - xi * sin
            ti = xr * sin + xi * cos
        first.append((er + tr, ei + ti))
        second.append((er - tr, ei - ti))
    return first + second


def place_of(wave):
    return 8 * (wave % 4) + wave // 4


def three_parts(x):
    high = x.astype(BF16)
    low = (x - high.astype(F32)).astype(BF16)
    return jnp.concatenate([high, low, high], axis=1)


def kernel(
    anomalies, increment, spectrum, forward_flip, forward, inverse, twist, out,
    anom, wide, incr, spec, turned, spec_flip, work, send_a, recv_a,
    column, send_b, recv_b, part, recv_part, pair, recv_pair,
    load_sem, send_a_sem, recv_a_sem, send_b_sem, recv_b_sem, part_sems, pair_sems, total_sems,
):
    me = lax.axis_index("slab")
    mem = lax.axis_index("mem")
    z, y, x = me // 8, (me // 2) % 4, me % 2
    core = mem % 2
    other_core = (mem // 2) * 2 + (1 - core)
    other_chip = (1 - mem // 2) * 2 + core

    def slab_at(offset):
        dz, dy, dx = offset
        return ((z + dz) % 4) * 8 + ((y + dy) % 4) * 2 + (x + dx) % 2

    def load_anomalies(b):
        rows = pl.ds(pl.multiple_of(b * 16, 16), 16)
        return pltpu.make_async_copy(anomalies.at[:, rows, :], anom.at[:, rows, :], load_sem.at[b])

    def load_increment(b):
        rows = pl.ds(pl.multiple_of(b * 16, 16), 16)
        return pltpu.make_async_copy(increment.at[rows, :], incr.at[rows, :], load_sem.at[8 + b])

    def start_loads(b, carry):
        load_anomalies(b).start()
        load_increment(b).start()
        return carry

    lax.fori_loop(0, 8, start_loads, 0)
    load_spectrum = pltpu.make_async_copy(spectrum, spec, load_sem.at[16])
    load_spectrum.start()

    barrier = pltpu.get_barrier_semaphore()
    for offset in OFFSETS:
        pl.semaphore_signal(
            barrier, inc=1, device_id={"mem": mem, "slab": slab_at(offset)}, device_id_type=MESH
        )
    for mate in (other_core, other_chip):
        pl.semaphore_signal(
            barrier, inc=1, device_id={"mem": mate, "slab": me}, device_id_type=MESH
        )

    sub = lax.broadcasted_iota(jnp.int32, (16, 8, 128), 1)
    lower = sub < 4

    def interlaced(a, b):
        even = jnp.where(lower, a, pltpu.roll(b, 4, 1))
        odd = jnp.where(lower, pltpu.roll(a, 4, 1), b)
        return even, odd

    def twisted(values, sign):
        result = [values[0]]
        for k in range(1, 32):
            re, im = values[k]
            cos, sin = twist[0, place_of(k)], twist[1, place_of(k)]
            if sign > 0:
                result.append((re * cos - im * sin, re * sin + im * cos))
            else:
                result.append((re * cos + im * sin, im * cos - re * sin))
        return result

    def first_step(b, carry):
        load_anomalies(b).wait()
        load_increment(b).wait()
        rows = pl.ds(pl.multiple_of(b * 16, 16), 16)
        for n in range(8):
            inputs = []
            for p in range(4):
                lanes = slice(128 * (n + 8 * p), 128 * (n + 8 * p) + 128)
                step = incr[rows, lanes]
                inputs.append(
                    (anom[0, rows, lanes].astype(F32) * step, anom[1, rows, lanes].astype(F32) * step)
                )
            for c, (re, im) in enumerate(short_transform(inputs, -1)):
                if c * n:
                    cos = math.cos(2.0 * math.pi * c * n / 32)
                    sin = -math.sin(2.0 * math.pi * c * n / 32)
                    re, im = re * cos - im * sin, re * sin + im * cos
                work[8 * c + n, rows, 0:128] = re
                work[8 * c + n, rows, 128:256] = im
        return carry

    lax.fori_loop(0, 8, first_step, 0)

    def send_copy(source, target, send_sem, recv_sem, chunk, slab):
        return pltpu.make_async_remote_copy(
            src_ref=source.at[chunk, slab],
            dst_ref=target.at[chunk, me],
            send_sem=send_sem.at[chunk],
            recv_sem=recv_sem.at[chunk],
            device_id={"mem": mem, "slab": slab},
            device_id_type=MESH,
        )

    def whole_copy(source, target, send_sem, recv_sem, chunk):
        return pltpu.make_async_remote_copy(
            src_ref=source.at[chunk, 0:31],
            dst_ref=target.at[chunk, 0:31],
            send_sem=send_sem.at[chunk],
            recv_sem=recv_sem.at[chunk],
            device_id={"mem": other_core, "slab": me},
            device_id_type=MESH,
        )

    def forward_class(chunk):
        def second_step(b, inner):
            rows = pl.ds(pl.multiple_of(b * 16, 16), 16)
            values = [
                (work[chunk * 8 + n, rows, 0:128], work[chunk * 8 + n, rows, 128:256])
                for n in range(8)
            ]
            for m, (re, im) in enumerate(short_transform(values, -1)):
                cos, sin = twist[0, chunk * 8 + m, 0:1, :], twist[1, chunk * 8 + m, 0:1, :]
                work[chunk * 8 + m, rows, 0:128] = re * cos + im * sin
                work[chunk * 8 + m, rows, 128:256] = im * cos - re * sin
            return inner

        lax.fori_loop(0, 8, second_step, 0)

        def one_pair(p, inner):
            first = pl.multiple_of(chunk * 8 + p * 2, 2)
            both = three_parts(work[pl.ds(first, 2)].reshape(256, 256))
            result = lax.dot_general(
                forward_flip[...], both, (((1,), (1,)), ((), ())), preferred_element_type=F32
            )
            rows = pl.ds(pl.multiple_of(p * 8, 8), 8)
            for part_at in range(2):
                piece = result[128 * part_at : 128 * part_at + 128]
                even, odd = interlaced(
                    piece[:, :128].reshape(16, 8, 128), piece[:, 128:].reshape(16, 8, 128)
                )
                for d in range(16):
                    send_a[chunk, 2 * d, part_at, rows, :] = even[d]
                    send_a[chunk, 2 * d + 1, part_at, rows, :] = odd[d]
            return inner

        lax.fori_loop(0, 4, one_pair, 0)

    def forward_send(chunk):
        for offset in OFFSETS:
            send_copy(send_a, recv_a, send_a_sem, recv_a_sem, chunk, slab_at(offset)).start()
        recv_a[chunk, me] = send_a[chunk, me]

    forward_class(0)
    pl.semaphore_wait(barrier, len(OFFSETS) + 2)
    forward_send(0)

    def forward_later(chunk, carry):
        forward_class(chunk)
        forward_send(chunk)
        return carry

    lax.fori_loop(1, 4, forward_later, 0)

    load_spectrum.wait()

    def flip_spectrum(k, carry):
        piece = spec[pl.ds(k, 128, stride=32), :] * (1.0 / (4096.0 * 4096.0))
        turned[...] = piece.T
        for c in range(4):
            for b in range(4):
                spec_flip[k, pl.ds(32 * c + b, 8, stride=4), :] = turned[
                    pl.ds(32 * b + c, 8, stride=4), :
                ]
        return carry

    lax.fori_loop(0, 32, flip_spectrum, 0)

    def widen(b, carry):
        rows = pl.ds(pl.multiple_of(b * 16, 16), 16)
        wide[:, rows, :] = anom[:, rows, :].astype(F32)
        return carry

    lax.fori_loop(0, 8, widen, 0)

    def columns(chunk, carry):
        whole_copy(send_a, recv_a, send_a_sem, recv_a_sem, chunk).wait_recv()

        def down(q, inner):
            rows = pl.ds(pl.multiple_of(q * 8, 8), 8)
            values = [
                (recv_a[chunk, s, 0, rows, :], recv_a[chunk, s, 1, rows, :]) for s in range(32)
            ]
            values = twisted(short_transform(values, -1), -1)
            for k in range(32):
                column[k, rows, 0:128] = values[k][0]
                column[k, rows, 128:256] = values[k][1]
            return inner

        lax.fori_loop(0, 4, down, 0)
        share = pl.ds(pl.multiple_of(chunk * 32, 32), 32)

        def across(g, inner):
            group = pl.ds(pl.multiple_of(g * 8, 8), 8)
            waves = jnp.dot(
                three_parts(column[group].reshape(256, 256)), forward[...],
                preferred_element_type=F32,
            )
            scale = spec_flip[group, share, :].reshape(256, 128)
            waves = jnp.concatenate([waves[:, :128] * scale, waves[:, 128:] * scale], axis=1)
            back = jnp.dot(three_parts(waves), inverse[...], preferred_element_type=F32)
            column[group] = back.reshape(8, 32, 256)
            return inner

        lax.fori_loop(0, 4, across, 0)

        def up(q, inner):
            rows = pl.ds(pl.multiple_of(q * 8, 8), 8)
            values = [(column[k, rows, 0:128], column[k, rows, 128:256]) for k in range(32)]
            values = short_transform(twisted(values, 1), 1)
            for s in range(32):
                send_b[chunk, s, 0, rows, :] = values[s][0]
                send_b[chunk, s, 1, rows, :] = values[s][1]
            return inner

        lax.fori_loop(0, 4, up, 0)
        for offset in OFFSETS:
            send_copy(send_b, recv_b, send_b_sem, recv_b_sem, chunk, slab_at(offset)).start()
        recv_b[chunk, me] = send_b[chunk, me]
        return carry

    lax.fori_loop(0, 4, columns, 0)

    def inverse_rows(chunk, carry):
        whole_copy(send_b, recv_b, send_b_sem, recv_b_sem, chunk).wait_recv()

        def one_pair(p, inner):
            rows = pl.ds(pl.multiple_of(p * 8, 8), 8)
            halves = []
            for part_at in range(2):
                even = jnp.stack([recv_b[chunk, 2 * d, part_at, rows, :] for d in range(16)])
                odd = jnp.stack([recv_b[chunk, 2 * d + 1, part_at, rows, :] for d in range(16)])
                a, b = interlaced(even, odd)
                halves.append((a.reshape(128, 128).T, b.reshape(128, 128).T))
            both = jnp.concatenate(
                [
                    jnp.concatenate([halves[0][i], halves[1][i]], axis=1)
                    for i in range(2)
                ],
                axis=0,
            )
            result = jnp.dot(three_parts(both), inverse[...], preferred_element_type=F32)
            for i in range(2):
                at = chunk * 8 + p * 2 + i
                cos, sin = twist[0, at, 0:1, :], twist[1, at, 0:1, :]
                re = result[128 * i : 128 * i + 128, :128]
                im = result[128 * i : 128 * i + 128, 128:]
                work[at, :, 0:128] = re * cos - im * sin
                work[at, :, 128:256] = re * sin + im * cos
            return inner

        lax.fori_loop(0, 4, one_pair, 0)
        return carry

    lax.fori_loop(0, 4, inverse_rows, 0)

    def member_sum(b):
        rows = pl.ds(pl.multiple_of(b * 8, 8), 8)
        values = [
            (work[place_of(a), rows, 0:128], work[place_of(a), rows, 128:256]) for a in range(32)
        ]
        for a, (re, im) in enumerate(short_transform(values, 1)):
            lanes = slice(128 * a, 128 * a + 128)
            part[b, :, lanes] = wide[0, rows, lanes] * re + wide[1, rows, lanes] * im

    def to_core(t):
        return pltpu.make_async_remote_copy(
            src_ref=part.at[2 * t + 1 - core],
            dst_ref=recv_part.at[t],
            send_sem=part_sems.at[0, t],
            recv_sem=part_sems.at[1, t],
            device_id={"mem": other_core, "slab": me},
            device_id_type=MESH,
        )

    def to_chip(t):
        return pltpu.make_async_remote_copy(
            src_ref=pair.at[t],
            dst_ref=recv_pair.at[t],
            send_sem=pair_sems.at[0, t],
            recv_sem=pair_sems.at[1, t],
            device_id={"mem": other_chip, "slab": me},
            device_id_type=MESH,
        )

    def block_rows(block):
        return pl.ds(pl.multiple_of(block * 8, 8), 8)

    def finished(t):
        rows = block_rows(2 * t + core)
        return pltpu.make_async_remote_copy(
            src_ref=out.at[rows, :],
            dst_ref=out.at[rows, :],
            send_sem=total_sems.at[0, t],
            recv_sem=total_sems.at[1, t],
            device_id={"mem": other_core, "slab": me},
            device_id_type=MESH,
        )

    def pass_on(t):
        to_core(t).wait_recv()
        pair[t] = part[2 * t + core] + recv_part[t]
        to_chip(t).start()

    def sum_and_send(t, carry):
        member_sum(2 * t + 1 - core)
        to_core(t).start()
        member_sum(2 * t + core)

        @pl.when(t >= 1)
        def _():
            pass_on(t - 1)

        return carry

    lax.fori_loop(0, 8, sum_and_send, 0)
    pass_on(7)

    def finish(t, carry):
        to_chip(t).wait_recv()
        out[block_rows(2 * t + core), :] = pair[t] + recv_pair[t]
        finished(t).start()
        return carry

    lax.fori_loop(0, 8, finish, 0)

    def drain_slab(t, carry):
        whole_copy(send_a, recv_a, send_a_sem, recv_a_sem, t).wait_send()
        whole_copy(send_b, recv_b, send_b_sem, recv_b_sem, t).wait_send()
        return carry

    lax.fori_loop(0, 4, drain_slab, 0)

    def drain(t, carry):
        to_core(t).wait_send()
        to_chip(t).wait_send()
        finished(t).wait_send()
        finished(t).wait_recv()
        return carry

    lax.fori_loop(0, 8, drain, 0)


def per_device(anomalies, increment, spectrum):
    tables, twist = constant_tables()
    vmem = pl.BlockSpec(memory_space=pltpu.VMEM)
    anywhere = pl.BlockSpec(memory_space=pl.ANY)
    dma = pltpu.SemaphoreType.DMA
    return pl.pallas_call(
        kernel,
        out_shape=pltpu.VMEM((128, 4096), F32),
        in_specs=[anywhere] * 3 + [vmem] * 4,
        out_specs=vmem,
        scratch_shapes=[
            pltpu.VMEM((2, 128, 4096), BF16),
            pltpu.VMEM((2, 128, 4096), F32),
            pltpu.VMEM((128, 4096), F32),
            pltpu.VMEM((4096, 128), F32),
            pltpu.VMEM((128, 128), F32),
            pltpu.VMEM((32, 128, 128), F32),
            pltpu.VMEM((32, 128, 256), F32),
            pltpu.VMEM((4, 32, 2, 32, 128), F32),
            pltpu.VMEM((4, 32, 2, 32, 128), F32),
            pltpu.VMEM((32, 32, 256), F32),
            pltpu.VMEM((4, 32, 2, 32, 128), F32),
            pltpu.VMEM((4, 32, 2, 32, 128), F32),
            pltpu.VMEM((16, 8, 4096), F32),
            pltpu.VMEM((8, 8, 4096), F32),
            pltpu.VMEM((8, 8, 4096), F32),
            pltpu.VMEM((8, 8, 4096), F32),
            dma((17,)),
            dma((4,)), dma((4,)), dma((4,)), dma((4,)),
            dma((2, 8)), dma((2, 8)), dma((2, 8)),
        ],
        compiler_params=pltpu.CompilerParams(
            collective_id=0, has_side_effects=True, vmem_limit_bytes=58 * 2**20
        ),
        name="covariance",
    )(anomalies, increment, spectrum, *[jnp.asarray(t) for t in tables], jnp.asarray(twist))


def solution(mesh):
    placed = (P("mem", "slab", None), P("slab", None), P(None, "slab"))
    return jax.shard_map(
        per_device, mesh=mesh, in_specs=placed, out_specs=P("slab", None), check_vma=False
    )
```

```python
import math

import jax
import jax.numpy as jnp
import numpy as np
from jax import lax
from jax.experimental import pallas as pl
from jax.experimental.pallas import tpu as pltpu
from jax.sharding import PartitionSpec as P

MESH = pl.DeviceIdType.MESH
F32 = jnp.float32
BF16 = jnp.bfloat16
ROOT_HALF = math.sqrt(0.5)

ROUNDS = (
    (2, 2), (1, 1), (3, 3), (0, 0), (1, 3), (3, 1), (0, 2), (2, 0),
    (1, 0), (3, 2), (1, 2), (3, 0), (0, 1), (2, 3), (2, 1), (0, 3),
)
OFFSETS = tuple(
    offset
    for a, b in ROUNDS
    for offset in ((a, b, 1), ((a + 2) % 4, (b + 2) % 4, 0))
    if offset != (0, 0, 0)
)


def constant_tables():
    index = np.arange(128)
    angle = 2.0 * np.pi / 128 * (np.outer(index, index) % 128)
    cos, sin = np.cos(angle), np.sin(angle)
    tables = []
    for sign in (-1.0, 1.0):
        block = np.block([[cos, sign * sin], [-sign * sin, cos]])
        if sign < 0:
            flipped = block.T
            high = flipped.astype(BF16)
            low = (flipped - high.astype(np.float64)).astype(BF16)
            tables.append(np.concatenate([high, high, low], axis=1))
        high = block.astype(BF16)
        low = (block - high.astype(np.float64)).astype(BF16)
        tables.append(np.concatenate([high, high, low], axis=0))
    order = np.arange(32) % 8 * 4 + np.arange(32) // 8
    twist = 2.0 * np.pi / 4096 * np.outer(order, index)
    twist = np.stack([np.cos(twist), np.sin(twist)]).astype(np.float32)
    twist = np.broadcast_to(twist[:, :, None, :], (2, 32, 8, 128)).copy()
    return tables, twist


def short_transform(values, sign):
    count = len(values)
    if count == 1:
        return values
    even = short_transform(values[0::2], sign)
    odd = short_transform(values[1::2], sign)
    first, second = [], []
    for k in range(count // 2):
        (er, ei), (xr, xi) = even[k], odd[k]
        if k == 0:
            tr, ti = xr, xi
        elif 4 * k == count:
            if sign > 0:
                first.append((er - xi, ei + xr))
                second.append((er + xi, ei - xr))
            else:
                first.append((er + xi, ei - xr))
                second.append((er - xi, ei + xr))
            continue
        elif 8 * k == count:
            tr = (xr - sign * xi if sign > 0 else xr + xi) * ROOT_HALF
            ti = (xi + xr if sign > 0 else xi - xr) * ROOT_HALF
        elif 8 * k == 3 * count:
            tr = (xr + xi if sign > 0 else xr - xi) * -ROOT_HALF
            ti = (xr - xi if sign > 0 else -xr - xi) * ROOT_HALF
        else:
            cos = math.cos(2.0 * math.pi * k / count)
            sin = sign * math.sin(2.0 * math.pi * k / count)
            tr = xr * cos - xi * sin
            ti = xr * sin + xi * cos
        first.append((er + tr, ei + ti))
        second.append((er - tr, ei - ti))
    return first + second


def place_of(wave):
    return 8 * (wave % 4) + wave // 4


def three_parts(x):
    high = x.astype(BF16)
    low = (x - high.astype(F32)).astype(BF16)
    return jnp.concatenate([high, low, high], axis=1)


def kernel(
    anomalies, increment, spectrum, flip_table, forward_table, inverse_table, twist_table, out,
    forward_flip, forward, inverse, twist,
    anom, wide, incr, spec, turned, spec_flip, work, send_a, recv_a,
    column, send_b, recv_b, part, recv_part, pair, recv_pair,
    load_sem, send_a_sem, recv_a_sem, send_b_sem, recv_b_sem, part_sems, pair_sems, total_sems,
):
    me = lax.axis_index("slab")
    mem = lax.axis_index("mem")
    z, y, x = me // 8, (me // 2) % 4, me % 2
    core = mem % 2
    other_core = (mem // 2) * 2 + (1 - core)
    other_chip = (1 - mem // 2) * 2 + core

    def slab_at(offset):
        dz, dy, dx = offset
        return ((z + dz) % 4) * 8 + ((y + dy) % 4) * 2 + (x + dx) % 2

    barrier = pltpu.get_barrier_semaphore()
    for offset in OFFSETS:
        pl.semaphore_signal(
            barrier, inc=1, device_id={"mem": mem, "slab": slab_at(offset)}, device_id_type=MESH
        )
    for mate in (other_core, other_chip):
        pl.semaphore_signal(
            barrier, inc=1, device_id={"mem": mate, "slab": me}, device_id_type=MESH
        )

    def load_anomalies(b):
        rows = pl.ds(pl.multiple_of(b * 16, 16), 16)
        return pltpu.make_async_copy(anomalies.at[:, rows, :], anom.at[:, rows, :], load_sem.at[b])

    def load_increment(b):
        rows = pl.ds(pl.multiple_of(b * 16, 16), 16)
        return pltpu.make_async_copy(increment.at[rows, :], incr.at[rows, :], load_sem.at[8 + b])

    def start_loads(b, carry):
        load_anomalies(b).start()
        load_increment(b).start()
        return carry

    load_twist = pltpu.make_async_copy(twist_table, twist, load_sem.at[17])
    load_flip = pltpu.make_async_copy(flip_table, forward_flip, load_sem.at[18])
    load_forward = pltpu.make_async_copy(forward_table, forward, load_sem.at[19])
    load_inverse = pltpu.make_async_copy(inverse_table, inverse, load_sem.at[20])
    load_spectrum = pltpu.make_async_copy(spectrum, spec, load_sem.at[16])
    lax.fori_loop(0, 8, start_loads, 0)
    for copy in (load_twist, load_flip, load_forward, load_inverse, load_spectrum):
        copy.start()

    sub = lax.broadcasted_iota(jnp.int32, (16, 8, 128), 1)
    lower = sub < 4

    def interlaced(a, b):
        even = jnp.where(lower, a, pltpu.roll(b, 4, 1))
        odd = jnp.where(lower, pltpu.roll(a, 4, 1), b)
        return even, odd

    def twisted(values, sign):
        result = [values[0]]
        for k in range(1, 32):
            re, im = values[k]
            cos, sin = twist[0, place_of(k)], twist[1, place_of(k)]
            if sign > 0:
                result.append((re * cos - im * sin, re * sin + im * cos))
            else:
                result.append((re * cos + im * sin, im * cos - re * sin))
        return result

    def first_step(b, carry):
        load_anomalies(b).wait()
        load_increment(b).wait()
        rows = pl.ds(pl.multiple_of(b * 16, 16), 16)
        for n in range(8):
            inputs = []
            for p in range(4):
                lanes = slice(128 * (n + 8 * p), 128 * (n + 8 * p) + 128)
                step = incr[rows, lanes]
                inputs.append(
                    (anom[0, rows, lanes].astype(F32) * step, anom[1, rows, lanes].astype(F32) * step)
                )
            for c, (re, im) in enumerate(short_transform(inputs, -1)):
                if c * n:
                    cos = math.cos(2.0 * math.pi * c * n / 32)
                    sin = -math.sin(2.0 * math.pi * c * n / 32)
                    re, im = re * cos - im * sin, re * sin + im * cos
                work[8 * c + n, rows, 0:128] = re
                work[8 * c + n, rows, 128:256] = im
        return carry

    lax.fori_loop(0, 8, first_step, 0)

    def send_copy(source, target, send_sem, recv_sem, chunk, slab):
        return pltpu.make_async_remote_copy(
            src_ref=source.at[chunk, slab],
            dst_ref=target.at[chunk, me],
            send_sem=send_sem.at[chunk],
            recv_sem=recv_sem.at[chunk],
            device_id={"mem": mem, "slab": slab},
            device_id_type=MESH,
        )

    def whole_copy(source, target, send_sem, recv_sem, chunk):
        return pltpu.make_async_remote_copy(
            src_ref=source.at[chunk, 0:31],
            dst_ref=target.at[chunk, 0:31],
            send_sem=send_sem.at[chunk],
            recv_sem=recv_sem.at[chunk],
            device_id={"mem": other_core, "slab": me},
            device_id_type=MESH,
        )

    def forward_class(chunk):
        def second_step(b, inner):
            rows = pl.ds(pl.multiple_of(b * 16, 16), 16)
            values = [
                (work[chunk * 8 + n, rows, 0:128], work[chunk * 8 + n, rows, 128:256])
                for n in range(8)
            ]
            for m, (re, im) in enumerate(short_transform(values, -1)):
                cos, sin = twist[0, chunk * 8 + m, 0:1, :], twist[1, chunk * 8 + m, 0:1, :]
                work[chunk * 8 + m, rows, 0:128] = re * cos + im * sin
                work[chunk * 8 + m, rows, 128:256] = im * cos - re * sin
            return inner

        lax.fori_loop(0, 8, second_step, 0)

        def one_pair(p, inner):
            first = pl.multiple_of(chunk * 8 + p * 2, 2)
            both = three_parts(work[pl.ds(first, 2)].reshape(256, 256))
            result = lax.dot_general(
                forward_flip[...], both, (((1,), (1,)), ((), ())), preferred_element_type=F32
            )
            rows = pl.ds(pl.multiple_of(p * 8, 8), 8)
            for part_at in range(2):
                piece = result[128 * part_at : 128 * part_at + 128]
                even, odd = interlaced(
                    piece[:, :128].reshape(16, 8, 128), piece[:, 128:].reshape(16, 8, 128)
                )
                for d in range(16):
                    send_a[chunk, 2 * d, part_at, rows, :] = even[d]
                    send_a[chunk, 2 * d + 1, part_at, rows, :] = odd[d]
            return inner

        lax.fori_loop(0, 4, one_pair, 0)

    def forward_send(chunk):
        for offset in OFFSETS:
            send_copy(send_a, recv_a, send_a_sem, recv_a_sem, chunk, slab_at(offset)).start()
        recv_a[chunk, me] = send_a[chunk, me]

    load_twist.wait()
    load_flip.wait()
    forward_class(0)
    pl.semaphore_wait(barrier, len(OFFSETS) + 2)
    forward_send(0)

    def forward_later(chunk, carry):
        forward_class(chunk)
        forward_send(chunk)
        return carry

    lax.fori_loop(1, 4, forward_later, 0)

    load_forward.wait()
    load_inverse.wait()
    load_spectrum.wait()

    def flip_spectrum(k, carry):
        piece = spec[pl.ds(k, 128, stride=32), :] * (1.0 / (4096.0 * 4096.0))
        turned[...] = piece.T
        for c in range(4):
            for b in range(4):
                spec_flip[k, pl.ds(32 * c + b, 8, stride=4), :] = turned[
                    pl.ds(32 * b + c, 8, stride=4), :
                ]
        return carry

    lax.fori_loop(0, 32, flip_spectrum, 0)

    def widen(b, carry):
        rows = pl.ds(pl.multiple_of(b * 16, 16), 16)
        wide[:, rows, :] = anom[:, rows, :].astype(F32)
        return carry

    lax.fori_loop(0, 8, widen, 0)

    def columns(chunk, carry):
        whole_copy(send_a, recv_a, send_a_sem, recv_a_sem, chunk).wait_recv()

        def down(q, inner):
            rows = pl.ds(pl.multiple_of(q * 8, 8), 8)
            values = [
                (recv_a[chunk, s, 0, rows, :], recv_a[chunk, s, 1, rows, :]) for s in range(32)
            ]
            values = twisted(short_transform(values, -1), -1)
            for k in range(32):
                column[k, rows, 0:128] = values[k][0]
                column[k, rows, 128:256] = values[k][1]
            return inner

        lax.fori_loop(0, 4, down, 0)
        share = pl.ds(pl.multiple_of(chunk * 32, 32), 32)

        def across(g, inner):
            group = pl.ds(pl.multiple_of(g * 8, 8), 8)
            waves = jnp.dot(
                three_parts(column[group].reshape(256, 256)), forward[...],
                preferred_element_type=F32,
            )
            scale = spec_flip[group, share, :].reshape(256, 128)
            waves = jnp.concatenate([waves[:, :128] * scale, waves[:, 128:] * scale], axis=1)
            back = jnp.dot(three_parts(waves), inverse[...], preferred_element_type=F32)
            column[group] = back.reshape(8, 32, 256)
            return inner

        lax.fori_loop(0, 4, across, 0)

        def up(q, inner):
            rows = pl.ds(pl.multiple_of(q * 8, 8), 8)
            values = [(column[k, rows, 0:128], column[k, rows, 128:256]) for k in range(32)]
            values = short_transform(twisted(values, 1), 1)
            for s in range(32):
                send_b[chunk, s, 0, rows, :] = values[s][0]
                send_b[chunk, s, 1, rows, :] = values[s][1]
            return inner

        lax.fori_loop(0, 4, up, 0)
        for offset in OFFSETS:
            send_copy(send_b, recv_b, send_b_sem, recv_b_sem, chunk, slab_at(offset)).start()
        recv_b[chunk, me] = send_b[chunk, me]
        return carry

    lax.fori_loop(0, 4, columns, 0)

    def inverse_rows(chunk, carry):
        whole_copy(send_b, recv_b, send_b_sem, recv_b_sem, chunk).wait_recv()

        def one_pair(p, inner):
            rows = pl.ds(pl.multiple_of(p * 8, 8), 8)
            halves = []
            for part_at in range(2):
                even = jnp.stack([recv_b[chunk, 2 * d, part_at, rows, :] for d in range(16)])
                odd = jnp.stack([recv_b[chunk, 2 * d + 1, part_at, rows, :] for d in range(16)])
                a, b = interlaced(even, odd)
                halves.append((a.reshape(128, 128).T, b.reshape(128, 128).T))
            both = jnp.concatenate(
                [
                    jnp.concatenate([halves[0][i], halves[1][i]], axis=1)
                    for i in range(2)
                ],
                axis=0,
            )
            result = jnp.dot(three_parts(both), inverse[...], preferred_element_type=F32)
            for i in range(2):
                at = chunk * 8 + p * 2 + i
                cos, sin = twist[0, at, 0:1, :], twist[1, at, 0:1, :]
                re = result[128 * i : 128 * i + 128, :128]
                im = result[128 * i : 128 * i + 128, 128:]
                work[at, :, 0:128] = re * cos - im * sin
                work[at, :, 128:256] = re * sin + im * cos
            return inner

        lax.fori_loop(0, 4, one_pair, 0)
        return carry

    lax.fori_loop(0, 4, inverse_rows, 0)

    def member_sum(b):
        rows = pl.ds(pl.multiple_of(b * 8, 8), 8)
        values = [
            (work[place_of(a), rows, 0:128], work[place_of(a), rows, 128:256]) for a in range(32)
        ]
        for a, (re, im) in enumerate(short_transform(values, 1)):
            lanes = slice(128 * a, 128 * a + 128)
            part[b, :, lanes] = wide[0, rows, lanes] * re + wide[1, rows, lanes] * im

    def to_core(t):
        return pltpu.make_async_remote_copy(
            src_ref=part.at[2 * t + 1 - core],
            dst_ref=recv_part.at[t],
            send_sem=part_sems.at[0, t],
            recv_sem=part_sems.at[1, t],
            device_id={"mem": other_core, "slab": me},
            device_id_type=MESH,
        )

    def to_chip(t):
        return pltpu.make_async_remote_copy(
            src_ref=pair.at[t],
            dst_ref=recv_pair.at[t],
            send_sem=pair_sems.at[0, t],
            recv_sem=pair_sems.at[1, t],
            device_id={"mem": other_chip, "slab": me},
            device_id_type=MESH,
        )

    def block_rows(block):
        return pl.ds(pl.multiple_of(block * 8, 8), 8)

    def finished(t):
        rows = block_rows(2 * t + core)
        return pltpu.make_async_remote_copy(
            src_ref=out.at[rows, :],
            dst_ref=out.at[rows, :],
            send_sem=total_sems.at[0, t],
            recv_sem=total_sems.at[1, t],
            device_id={"mem": other_core, "slab": me},
            device_id_type=MESH,
        )

    def pass_on(t):
        to_core(t).wait_recv()
        pair[t] = part[2 * t + core] + recv_part[t]
        to_chip(t).start()

    def sum_and_send(t, carry):
        member_sum(2 * t + 1 - core)
        to_core(t).start()
        member_sum(2 * t + core)

        @pl.when(t >= 1)
        def _():
            pass_on(t - 1)

        return carry

    lax.fori_loop(0, 8, sum_and_send, 0)
    pass_on(7)

    def finish(t, carry):
        to_chip(t).wait_recv()
        out[block_rows(2 * t + core), :] = pair[t] + recv_pair[t]
        finished(t).start()
        return carry

    lax.fori_loop(0, 8, finish, 0)

    def drain_slab(t, carry):
        whole_copy(send_a, recv_a, send_a_sem, recv_a_sem, t).wait_send()
        whole_copy(send_b, recv_b, send_b_sem, recv_b_sem, t).wait_send()
        return carry

    lax.fori_loop(0, 4, drain_slab, 0)

    def drain(t, carry):
        to_core(t).wait_send()
        to_chip(t).wait_send()
        finished(t).wait_send()
        finished(t).wait_recv()
        return carry

    lax.fori_loop(0, 8, drain, 0)


def per_device(anomalies, increment, spectrum):
    tables, twist = constant_tables()
    vmem = pl.BlockSpec(memory_space=pltpu.VMEM)
    anywhere = pl.BlockSpec(memory_space=pl.ANY)
    dma = pltpu.SemaphoreType.DMA
    return pl.pallas_call(
        kernel,
        out_shape=pltpu.VMEM((128, 4096), F32),
        in_specs=[anywhere] * 7,
        out_specs=vmem,
        scratch_shapes=[
            pltpu.VMEM((256, 768), BF16),
            pltpu.VMEM((768, 256), BF16),
            pltpu.VMEM((768, 256), BF16),
            pltpu.VMEM((2, 32, 8, 128), F32),
            pltpu.VMEM((2, 128, 4096), BF16),
            pltpu.VMEM((2, 128, 4096), F32),
            pltpu.VMEM((128, 4096), F32),
            pltpu.VMEM((4096, 128), F32),
            pltpu.VMEM((128, 128), F32),
            pltpu.VMEM((32, 128, 128), F32),
            pltpu.VMEM((32, 128, 256), F32),
            pltpu.VMEM((4, 32, 2, 32, 128), F32),
            pltpu.VMEM((4, 32, 2, 32, 128), F32),
            pltpu.VMEM((32, 32, 256), F32),
            pltpu.VMEM((4, 32, 2, 32, 128), F32),
            pltpu.VMEM((4, 32, 2, 32, 128), F32),
            pltpu.VMEM((16, 8, 4096), F32),
            pltpu.VMEM((8, 8, 4096), F32),
            pltpu.VMEM((8, 8, 4096), F32),
            pltpu.VMEM((8, 8, 4096), F32),
            dma((21,)),
            dma((4,)), dma((4,)), dma((4,)), dma((4,)),
            dma((2, 8)), dma((2, 8)), dma((2, 8)),
        ],
        compiler_params=pltpu.CompilerParams(
            collective_id=0, has_side_effects=True, vmem_limit_bytes=58 * 2**20
        ),
        name="covariance",
    )(anomalies, increment, spectrum, *[jnp.asarray(t) for t in tables], jnp.asarray(twist))


def solution(mesh):
    placed = (P("mem", "slab", None), P("slab", None), P(None, "slab"))
    return jax.shard_map(
        per_device, mesh=mesh, in_specs=placed, out_specs=P("slab", None), check_vma=False
    )
```

```python
import math

import jax
import jax.numpy as jnp
import numpy as np
from jax import lax
from jax.experimental import pallas as pl
from jax.experimental.pallas import tpu as pltpu
from jax.sharding import PartitionSpec as P

MESH = pl.DeviceIdType.MESH
F32 = jnp.float32
BF16 = jnp.bfloat16
ROOT_HALF = math.sqrt(0.5)
CLASSES = 8
SIZE = 32 // CLASSES
ROWS = 4 * SIZE

ROUNDS = (
    (2, 2), (1, 1), (3, 3), (0, 0), (1, 3), (3, 1), (0, 2), (2, 0),
    (1, 0), (3, 2), (1, 2), (3, 0), (0, 1), (2, 3), (2, 1), (0, 3),
)
OFFSETS = tuple(
    offset
    for a, b in ROUNDS
    for offset in ((a, b, 1), ((a + 2) % 4, (b + 2) % 4, 0))
    if offset != (0, 0, 0)
)


def constant_tables():
    index = np.arange(128)
    angle = 2.0 * np.pi / 128 * (np.outer(index, index) % 128)
    cos, sin = np.cos(angle), np.sin(angle)
    tables = []
    for sign in (-1.0, 1.0):
        block = np.block([[cos, sign * sin], [-sign * sin, cos]])
        if sign < 0:
            flipped = block.T
            high = flipped.astype(BF16)
            low = (flipped - high.astype(np.float64)).astype(BF16)
            tables.append(np.concatenate([high, high, low], axis=1))
        high = block.astype(BF16)
        low = (block - high.astype(np.float64)).astype(BF16)
        tables.append(np.concatenate([high, high, low], axis=0))
    order = np.arange(32) % SIZE * CLASSES + np.arange(32) // SIZE
    twist = 2.0 * np.pi / 4096 * np.outer(order, index)
    twist = np.stack([np.cos(twist), np.sin(twist)]).astype(np.float32)
    twist = np.broadcast_to(twist[:, :, None, :], (2, 32, 8, 128)).copy()
    return tables, twist


def short_transform(values, sign):
    count = len(values)
    if count == 1:
        return values
    even = short_transform(values[0::2], sign)
    odd = short_transform(values[1::2], sign)
    first, second = [], []
    for k in range(count // 2):
        (er, ei), (xr, xi) = even[k], odd[k]
        if k == 0:
            tr, ti = xr, xi
        elif 4 * k == count:
            if sign > 0:
                first.append((er - xi, ei + xr))
                second.append((er + xi, ei - xr))
            else:
                first.append((er + xi, ei - xr))
                second.append((er - xi, ei + xr))
            continue
        elif 8 * k == count:
            tr = (xr - sign * xi if sign > 0 else xr + xi) * ROOT_HALF
            ti = (xi + xr if sign > 0 else xi - xr) * ROOT_HALF
        elif 8 * k == 3 * count:
            tr = (xr + xi if sign > 0 else xr - xi) * -ROOT_HALF
            ti = (xr - xi if sign > 0 else -xr - xi) * ROOT_HALF
        else:
            cos = math.cos(2.0 * math.pi * k / count)
            sin = sign * math.sin(2.0 * math.pi * k / count)
            tr = xr * cos - xi * sin
            ti = xr * sin + xi * cos
        first.append((er + tr, ei + ti))
        second.append((er - tr, ei - ti))
    return first + second


def place_of(wave):
    return SIZE * (wave % CLASSES) + wave // CLASSES


def three_parts(x):
    high = x.astype(BF16)
    low = (x - high.astype(F32)).astype(BF16)
    return jnp.concatenate([high, low, high], axis=1)


def kernel(
    anomalies, increment, spectrum, flip_table, forward_table, inverse_table, twist_table, out,
    forward_flip, forward, inverse, twist,
    anom, wide, incr, spec, turned, spec_flip, work, send_a, recv_a,
    column, send_b, recv_b, part, recv_part, pair, recv_pair,
    load_sem, send_a_sem, recv_a_sem, send_b_sem, recv_b_sem, part_sems, pair_sems, total_sems,
):
    me = lax.axis_index("slab")
    mem = lax.axis_index("mem")
    z, y, x = me // 8, (me // 2) % 4, me % 2
    core = mem % 2
    other_core = (mem // 2) * 2 + (1 - core)
    other_chip = (1 - mem // 2) * 2 + core

    def slab_at(offset):
        dz, dy, dx = offset
        return ((z + dz) % 4) * 8 + ((y + dy) % 4) * 2 + (x + dx) % 2

    barrier = pltpu.get_barrier_semaphore()
    for offset in OFFSETS:
        pl.semaphore_signal(
            barrier, inc=1, device_id={"mem": mem, "slab": slab_at(offset)}, device_id_type=MESH
        )
    for mate in (other_core, other_chip):
        pl.semaphore_signal(
            barrier, inc=1, device_id={"mem": mate, "slab": me}, device_id_type=MESH
        )

    def load_anomalies(b):
        rows = pl.ds(pl.multiple_of(b * 16, 16), 16)
        return pltpu.make_async_copy(anomalies.at[:, rows, :], anom.at[:, rows, :], load_sem.at[b])

    def load_increment(b):
        rows = pl.ds(pl.multiple_of(b * 16, 16), 16)
        return pltpu.make_async_copy(increment.at[rows, :], incr.at[rows, :], load_sem.at[8 + b])

    def start_loads(b, carry):
        load_anomalies(b).start()
        load_increment(b).start()
        return carry

    load_twist = pltpu.make_async_copy(twist_table, twist, load_sem.at[17])
    load_flip = pltpu.make_async_copy(flip_table, forward_flip, load_sem.at[18])
    load_forward = pltpu.make_async_copy(forward_table, forward, load_sem.at[19])
    load_inverse = pltpu.make_async_copy(inverse_table, inverse, load_sem.at[20])
    load_spectrum = pltpu.make_async_copy(spectrum, spec, load_sem.at[16])
    lax.fori_loop(0, 8, start_loads, 0)
    for copy in (load_twist, load_flip, load_forward, load_inverse, load_spectrum):
        copy.start()

    sub = lax.broadcasted_iota(jnp.int32, (16, 8, 128), 1)
    lower = sub < 4

    def interlaced(a, b):
        even = jnp.where(lower, a, pltpu.roll(b, 4, 1))
        odd = jnp.where(lower, pltpu.roll(a, 4, 1), b)
        return even, odd

    def twisted(values, sign):
        result = [values[0]]
        for k in range(1, 32):
            re, im = values[k]
            cos, sin = twist[0, place_of(k)], twist[1, place_of(k)]
            if sign > 0:
                result.append((re * cos - im * sin, re * sin + im * cos))
            else:
                result.append((re * cos + im * sin, im * cos - re * sin))
        return result

    def first_step(b, carry):
        load_anomalies(b).wait()
        load_increment(b).wait()
        rows = pl.ds(pl.multiple_of(b * 16, 16), 16)
        for n in range(SIZE):
            inputs = []
            for p in range(CLASSES):
                lanes = slice(128 * (n + SIZE * p), 128 * (n + SIZE * p) + 128)
                step = incr[rows, lanes]
                inputs.append(
                    (anom[0, rows, lanes].astype(F32) * step, anom[1, rows, lanes].astype(F32) * step)
                )
            for c, (re, im) in enumerate(short_transform(inputs, -1)):
                if c * n:
                    cos = math.cos(2.0 * math.pi * c * n / 32)
                    sin = -math.sin(2.0 * math.pi * c * n / 32)
                    re, im = re * cos - im * sin, re * sin + im * cos
                work[SIZE * c + n, rows, 0:128] = re
                work[SIZE * c + n, rows, 128:256] = im
        return carry

    lax.fori_loop(0, 8, first_step, 0)

    def send_copy(source, target, send_sem, recv_sem, chunk, slab):
        return pltpu.make_async_remote_copy(
            src_ref=source.at[chunk, slab],
            dst_ref=target.at[chunk, me],
            send_sem=send_sem.at[chunk],
            recv_sem=recv_sem.at[chunk],
            device_id={"mem": mem, "slab": slab},
            device_id_type=MESH,
        )

    def whole_copy(source, target, send_sem, recv_sem, chunk):
        return pltpu.make_async_remote_copy(
            src_ref=source.at[chunk, 0:31],
            dst_ref=target.at[chunk, 0:31],
            send_sem=send_sem.at[chunk],
            recv_sem=recv_sem.at[chunk],
            device_id={"mem": other_core, "slab": me},
            device_id_type=MESH,
        )

    def forward_class(chunk):
        def second_step(b, inner):
            rows = pl.ds(pl.multiple_of(b * 16, 16), 16)
            values = [
                (work[chunk * SIZE + n, rows, 0:128], work[chunk * SIZE + n, rows, 128:256])
                for n in range(SIZE)
            ]
            for m, (re, im) in enumerate(short_transform(values, -1)):
                at = chunk * SIZE + m
                cos, sin = twist[0, at, 0:1, :], twist[1, at, 0:1, :]
                work[at, rows, 0:128] = re * cos + im * sin
                work[at, rows, 128:256] = im * cos - re * sin
            return inner

        lax.fori_loop(0, 8, second_step, 0)

        def one_pair(p, inner):
            first = pl.multiple_of(chunk * SIZE + p * 2, 2)
            both = three_parts(work[pl.ds(first, 2)].reshape(256, 256))
            result = lax.dot_general(
                forward_flip[...], both, (((1,), (1,)), ((), ())), preferred_element_type=F32
            )
            rows = pl.ds(pl.multiple_of(p * 8, 8), 8)
            for part_at in range(2):
                piece = result[128 * part_at : 128 * part_at + 128]
                even, odd = interlaced(
                    piece[:, :128].reshape(16, 8, 128), piece[:, 128:].reshape(16, 8, 128)
                )
                for d in range(16):
                    send_a[chunk, 2 * d, part_at, rows, :] = even[d]
                    send_a[chunk, 2 * d + 1, part_at, rows, :] = odd[d]
            return inner

        lax.fori_loop(0, SIZE // 2, one_pair, 0)

    def forward_send(chunk):
        for offset in OFFSETS:
            send_copy(send_a, recv_a, send_a_sem, recv_a_sem, chunk, slab_at(offset)).start()
        recv_a[chunk, me] = send_a[chunk, me]

    load_twist.wait()
    load_flip.wait()
    forward_class(0)
    pl.semaphore_wait(barrier, len(OFFSETS) + 2)
    forward_send(0)

    def forward_later(chunk, carry):
        forward_class(chunk)
        forward_send(chunk)
        return carry

    lax.fori_loop(1, CLASSES, forward_later, 0)

    load_forward.wait()
    load_inverse.wait()
    load_spectrum.wait()

    def flip_spectrum(k, carry):
        piece = spec[pl.ds(k, 128, stride=32), :] * (1.0 / (4096.0 * 4096.0))
        turned[...] = piece.T
        for c in range(CLASSES):
            for b in range(4):
                spec_flip[k, pl.ds(ROWS * c + b, SIZE, stride=4), :] = turned[
                    pl.ds(32 * b + c, SIZE, stride=CLASSES), :
                ]
        return carry

    lax.fori_loop(0, 32, flip_spectrum, 0)

    def widen(b, carry):
        rows = pl.ds(pl.multiple_of(b * 16, 16), 16)
        wide[:, rows, :] = anom[:, rows, :].astype(F32)
        return carry

    lax.fori_loop(0, 8, widen, 0)

    def columns(chunk, carry):
        whole_copy(send_a, recv_a, send_a_sem, recv_a_sem, chunk).wait_recv()

        def down(q, inner):
            rows = pl.ds(pl.multiple_of(q * 8, 8), 8)
            values = [
                (recv_a[chunk, s, 0, rows, :], recv_a[chunk, s, 1, rows, :]) for s in range(32)
            ]
            values = twisted(short_transform(values, -1), -1)
            for k in range(32):
                column[k, rows, 0:128] = values[k][0]
                column[k, rows, 128:256] = values[k][1]
            return inner

        lax.fori_loop(0, ROWS // 8, down, 0)
        share = pl.ds(pl.multiple_of(chunk * ROWS, ROWS), ROWS)

        def across(g, inner):
            group = pl.ds(pl.multiple_of(g * 256 // ROWS, 256 // ROWS), 256 // ROWS)
            waves = jnp.dot(
                three_parts(column[group].reshape(256, 256)), forward[...],
                preferred_element_type=F32,
            )
            scale = spec_flip[group, share, :].reshape(256, 128)
            waves = jnp.concatenate([waves[:, :128] * scale, waves[:, 128:] * scale], axis=1)
            back = jnp.dot(three_parts(waves), inverse[...], preferred_element_type=F32)
            column[group] = back.reshape(256 // ROWS, ROWS, 256)
            return inner

        lax.fori_loop(0, ROWS // 8, across, 0)

        def up(q, inner):
            rows = pl.ds(pl.multiple_of(q * 8, 8), 8)
            values = [(column[k, rows, 0:128], column[k, rows, 128:256]) for k in range(32)]
            values = short_transform(twisted(values, 1), 1)
            for s in range(32):
                send_b[chunk, s, 0, rows, :] = values[s][0]
                send_b[chunk, s, 1, rows, :] = values[s][1]
            return inner

        lax.fori_loop(0, ROWS // 8, up, 0)
        for offset in OFFSETS:
            send_copy(send_b, recv_b, send_b_sem, recv_b_sem, chunk, slab_at(offset)).start()
        recv_b[chunk, me] = send_b[chunk, me]
        return carry

    lax.fori_loop(0, CLASSES, columns, 0)

    def inverse_rows(chunk, carry):
        whole_copy(send_b, recv_b, send_b_sem, recv_b_sem, chunk).wait_recv()

        def one_pair(p, inner):
            rows = pl.ds(pl.multiple_of(p * 8, 8), 8)
            halves = []
            for part_at in range(2):
                even = jnp.stack([recv_b[chunk, 2 * d, part_at, rows, :] for d in range(16)])
                odd = jnp.stack([recv_b[chunk, 2 * d + 1, part_at, rows, :] for d in range(16)])
                a, b = interlaced(even, odd)
                halves.append((a.reshape(128, 128).T, b.reshape(128, 128).T))
            both = jnp.concatenate(
                [
                    jnp.concatenate([halves[0][i], halves[1][i]], axis=1)
                    for i in range(2)
                ],
                axis=0,
            )
            result = jnp.dot(three_parts(both), inverse[...], preferred_element_type=F32)
            for i in range(2):
                at = chunk * SIZE + p * 2 + i
                cos, sin = twist[0, at, 0:1, :], twist[1, at, 0:1, :]
                re = result[128 * i : 128 * i + 128, :128]
                im = result[128 * i : 128 * i + 128, 128:]
                work[at, :, 0:128] = re * cos - im * sin
                work[at, :, 128:256] = re * sin + im * cos
            return inner

        lax.fori_loop(0, SIZE // 2, one_pair, 0)
        return carry

    lax.fori_loop(0, CLASSES, inverse_rows, 0)

    def member_sum(b):
        rows = pl.ds(pl.multiple_of(b * 8, 8), 8)
        values = [
            (work[place_of(a), rows, 0:128], work[place_of(a), rows, 128:256]) for a in range(32)
        ]
        for a, (re, im) in enumerate(short_transform(values, 1)):
            lanes = slice(128 * a, 128 * a + 128)
            part[b, :, lanes] = wide[0, rows, lanes] * re + wide[1, rows, lanes] * im

    def to_core(t):
        return pltpu.make_async_remote_copy(
            src_ref=part.at[2 * t + 1 - core],
            dst_ref=recv_part.at[t],
            send_sem=part_sems.at[0, t],
            recv_sem=part_sems.at[1, t],
            device_id={"mem": other_core, "slab": me},
            device_id_type=MESH,
        )

    def to_chip(t):
        return pltpu.make_async_remote_copy(
            src_ref=pair.at[t],
            dst_ref=recv_pair.at[t],
            send_sem=pair_sems.at[0, t],
            recv_sem=pair_sems.at[1, t],
            device_id={"mem": other_chip, "slab": me},
            device_id_type=MESH,
        )

    def block_rows(block):
        return pl.ds(pl.multiple_of(block * 8, 8), 8)

    def finished(t):
        rows = block_rows(2 * t + core)
        return pltpu.make_async_remote_copy(
            src_ref=out.at[rows, :],
            dst_ref=out.at[rows, :],
            send_sem=total_sems.at[0, t],
            recv_sem=total_sems.at[1, t],
            device_id={"mem": other_core, "slab": me},
            device_id_type=MESH,
        )

    def pass_on(t):
        to_core(t).wait_recv()
        pair[t] = part[2 * t + core] + recv_part[t]
        to_chip(t).start()

    def sum_and_send(t, carry):
        member_sum(2 * t + 1 - core)
        to_core(t).start()
        member_sum(2 * t + core)

        @pl.when(t >= 1)
        def _():
            pass_on(t - 1)

        return carry

    lax.fori_loop(0, 8, sum_and_send, 0)
    pass_on(7)

    def finish(t, carry):
        to_chip(t).wait_recv()
        out[block_rows(2 * t + core), :] = pair[t] + recv_pair[t]
        finished(t).start()
        return carry

    lax.fori_loop(0, 8, finish, 0)

    def drain_slab(t, carry):
        whole_copy(send_a, recv_a, send_a_sem, recv_a_sem, t).wait_send()
        whole_copy(send_b, recv_b, send_b_sem, recv_b_sem, t).wait_send()
        return carry

    lax.fori_loop(0, CLASSES, drain_slab, 0)

    def drain(t, carry):
        to_core(t).wait_send()
        to_chip(t).wait_send()
        finished(t).wait_send()
        finished(t).wait_recv()
        return carry

    lax.fori_loop(0, 8, drain, 0)


def per_device(anomalies, increment, spectrum):
    tables, twist = constant_tables()
    vmem = pl.BlockSpec(memory_space=pltpu.VMEM)
    anywhere = pl.BlockSpec(memory_space=pl.ANY)
    dma = pltpu.SemaphoreType.DMA
    return pl.pallas_call(
        kernel,
        out_shape=pltpu.VMEM((128, 4096), F32),
        in_specs=[anywhere] * 7,
        out_specs=vmem,
        scratch_shapes=[
            pltpu.VMEM((256, 768), BF16),
            pltpu.VMEM((768, 256), BF16),
            pltpu.VMEM((768, 256), BF16),
            pltpu.VMEM((2, 32, 8, 128), F32),
            pltpu.VMEM((2, 128, 4096), BF16),
            pltpu.VMEM((2, 128, 4096), F32),
            pltpu.VMEM((128, 4096), F32),
            pltpu.VMEM((4096, 128), F32),
            pltpu.VMEM((128, 128), F32),
            pltpu.VMEM((32, 128, 128), F32),
            pltpu.VMEM((32, 128, 256), F32),
            pltpu.VMEM((CLASSES, 32, 2, ROWS, 128), F32),
            pltpu.VMEM((CLASSES, 32, 2, ROWS, 128), F32),
            pltpu.VMEM((32, ROWS, 256), F32),
            pltpu.VMEM((CLASSES, 32, 2, ROWS, 128), F32),
            pltpu.VMEM((CLASSES, 32, 2, ROWS, 128), F32),
            pltpu.VMEM((16, 8, 4096), F32),
            pltpu.VMEM((8, 8, 4096), F32),
            pltpu.VMEM((8, 8, 4096), F32),
            pltpu.VMEM((8, 8, 4096), F32),
            dma((21,)),
            dma((CLASSES,)), dma((CLASSES,)), dma((CLASSES,)), dma((CLASSES,)),
            dma((2, 8)), dma((2, 8)), dma((2, 8)),
        ],
        compiler_params=pltpu.CompilerParams(
            collective_id=0, has_side_effects=True, vmem_limit_bytes=58 * 2**20
        ),
        name="covariance",
    )(anomalies, increment, spectrum, *[jnp.asarray(t) for t in tables], jnp.asarray(twist))


def solution(mesh):
    placed = (P("mem", "slab", None), P("slab", None), P(None, "slab"))
    return jax.shard_map(
        per_device, mesh=mesh, in_specs=placed, out_specs=P("slab", None), check_vma=False
    )
```

```python
import math

import jax
import jax.numpy as jnp
import numpy as np
from jax import lax
from jax.experimental import pallas as pl
from jax.experimental.pallas import tpu as pltpu
from jax.sharding import PartitionSpec as P

MESH = pl.DeviceIdType.MESH
F32 = jnp.float32
BF16 = jnp.bfloat16
ROOT_HALF = math.sqrt(0.5)
CLASSES = 8
SIZE = 32 // CLASSES
DEFERRED = 3
ROWS = 4 * SIZE

ROUNDS = (
    (2, 2), (1, 1), (3, 3), (0, 0), (1, 3), (3, 1), (0, 2), (2, 0),
    (1, 0), (3, 2), (1, 2), (3, 0), (0, 1), (2, 3), (2, 1), (0, 3),
)
OFFSETS = tuple(
    offset
    for a, b in ROUNDS
    for offset in ((a, b, 1), ((a + 2) % 4, (b + 2) % 4, 0))
    if offset != (0, 0, 0)
)


def constant_tables():
    index = np.arange(128)
    angle = 2.0 * np.pi / 128 * (np.outer(index, index) % 128)
    cos, sin = np.cos(angle), np.sin(angle)
    tables = []
    for sign in (-1.0, 1.0):
        block = np.block([[cos, sign * sin], [-sign * sin, cos]])
        if sign < 0:
            flipped = block.T
            high = flipped.astype(BF16)
            low = (flipped - high.astype(np.float64)).astype(BF16)
            tables.append(np.concatenate([high, high, low], axis=1))
        high = block.astype(BF16)
        low = (block - high.astype(np.float64)).astype(BF16)
        tables.append(np.concatenate([high, high, low], axis=0))
    order = np.arange(32) % SIZE * CLASSES + np.arange(32) // SIZE
    twist = 2.0 * np.pi / 4096 * np.outer(order, index)
    twist = np.stack([np.cos(twist), np.sin(twist)]).astype(np.float32)
    twist = np.broadcast_to(twist[:, :, None, :], (2, 32, 8, 128)).copy()
    return tables, twist


def short_transform(values, sign):
    count = len(values)
    if count == 1:
        return values
    even = short_transform(values[0::2], sign)
    odd = short_transform(values[1::2], sign)
    first, second = [], []
    for k in range(count // 2):
        (er, ei), (xr, xi) = even[k], odd[k]
        if k == 0:
            tr, ti = xr, xi
        elif 4 * k == count:
            if sign > 0:
                first.append((er - xi, ei + xr))
                second.append((er + xi, ei - xr))
            else:
                first.append((er + xi, ei - xr))
                second.append((er - xi, ei + xr))
            continue
        elif 8 * k == count:
            tr = (xr - sign * xi if sign > 0 else xr + xi) * ROOT_HALF
            ti = (xi + xr if sign > 0 else xi - xr) * ROOT_HALF
        elif 8 * k == 3 * count:
            tr = (xr + xi if sign > 0 else xr - xi) * -ROOT_HALF
            ti = (xr - xi if sign > 0 else -xr - xi) * ROOT_HALF
        else:
            cos = math.cos(2.0 * math.pi * k / count)
            sin = sign * math.sin(2.0 * math.pi * k / count)
            tr = xr * cos - xi * sin
            ti = xr * sin + xi * cos
        first.append((er + tr, ei + ti))
        second.append((er - tr, ei - ti))
    return first + second


def place_of(wave):
    return SIZE * (wave % CLASSES) + wave // CLASSES


def three_parts(x):
    high = x.astype(BF16)
    low = (x - high.astype(F32)).astype(BF16)
    return jnp.concatenate([high, low, high], axis=1)


def kernel(
    anomalies, increment, spectrum, flip_table, forward_table, inverse_table, twist_table, out,
    forward_flip, forward, inverse, twist,
    anom, wide, incr, spec, turned, spec_flip, work, send_a, recv_a,
    column, staged, send_b, recv_b, part, recv_part, pair, recv_pair,
    load_sem, send_a_sem, recv_a_sem, send_b_sem, recv_b_sem, half_sems, part_sems, pair_sems, total_sems,
):
    me = lax.axis_index("slab")
    mem = lax.axis_index("mem")
    z, y, x = me // 8, (me // 2) % 4, me % 2
    core = mem % 2
    other_core = (mem // 2) * 2 + (1 - core)
    other_chip = (1 - mem // 2) * 2 + core

    def slab_at(offset):
        dz, dy, dx = offset
        return ((z + dz) % 4) * 8 + ((y + dy) % 4) * 2 + (x + dx) % 2

    barrier = pltpu.get_barrier_semaphore()
    for offset in OFFSETS:
        pl.semaphore_signal(
            barrier, inc=1, device_id={"mem": mem, "slab": slab_at(offset)}, device_id_type=MESH
        )
    for mate in (other_core, other_chip):
        pl.semaphore_signal(
            barrier, inc=1, device_id={"mem": mate, "slab": me}, device_id_type=MESH
        )

    def load_anomalies(b):
        rows = pl.ds(pl.multiple_of(b * 16, 16), 16)
        return pltpu.make_async_copy(anomalies.at[:, rows, :], anom.at[:, rows, :], load_sem.at[b])

    def load_increment(b):
        rows = pl.ds(pl.multiple_of(b * 16, 16), 16)
        return pltpu.make_async_copy(increment.at[rows, :], incr.at[rows, :], load_sem.at[8 + b])

    def start_loads(b, carry):
        load_anomalies(b).start()
        load_increment(b).start()
        return carry

    load_twist = pltpu.make_async_copy(twist_table, twist, load_sem.at[17])
    load_flip = pltpu.make_async_copy(flip_table, forward_flip, load_sem.at[18])
    load_forward = pltpu.make_async_copy(forward_table, forward, load_sem.at[19])
    load_inverse = pltpu.make_async_copy(inverse_table, inverse, load_sem.at[20])
    load_spectrum = pltpu.make_async_copy(spectrum, spec, load_sem.at[16])
    lax.fori_loop(0, 8, start_loads, 0)
    for copy in (load_twist, load_flip, load_forward, load_inverse, load_spectrum):
        copy.start()

    sub = lax.broadcasted_iota(jnp.int32, (16, 8, 128), 1)
    lower = sub < 4
    left = lax.broadcasted_iota(jnp.int32, (8, 128), 1) < 64

    def interlaced(a, b):
        even = jnp.where(lower, a, pltpu.roll(b, 4, 1))
        odd = jnp.where(lower, pltpu.roll(a, 4, 1), b)
        return even, odd

    def twisted(values, sign):
        result = [values[0]]
        for k in range(1, 32):
            re, im = values[k]
            cos, sin = twist[0, place_of(k)], twist[1, place_of(k)]
            if sign > 0:
                result.append((re * cos - im * sin, re * sin + im * cos))
            else:
                result.append((re * cos + im * sin, im * cos - re * sin))
        return result

    def first_step(b, carry):
        load_anomalies(b).wait()
        load_increment(b).wait()
        rows = pl.ds(pl.multiple_of(b * 16, 16), 16)
        for n in range(SIZE):
            inputs = []
            for p in range(CLASSES):
                lanes = slice(128 * (n + SIZE * p), 128 * (n + SIZE * p) + 128)
                step = incr[rows, lanes]
                inputs.append(
                    (anom[0, rows, lanes].astype(F32) * step, anom[1, rows, lanes].astype(F32) * step)
                )
            for c, (re, im) in enumerate(short_transform(inputs, -1)):
                if c * n:
                    cos = math.cos(2.0 * math.pi * c * n / 32)
                    sin = -math.sin(2.0 * math.pi * c * n / 32)
                    re, im = re * cos - im * sin, re * sin + im * cos
                work[SIZE * c + n, rows, 0:128] = re
                work[SIZE * c + n, rows, 128:256] = im
        return carry

    lax.fori_loop(0, 8, first_step, 0)

    def send_copy(source, target, send_sem, recv_sem, chunk, slab):
        return pltpu.make_async_remote_copy(
            src_ref=source.at[chunk, slab],
            dst_ref=target.at[chunk, me],
            send_sem=send_sem.at[chunk],
            recv_sem=recv_sem.at[chunk],
            device_id={"mem": mem, "slab": slab},
            device_id_type=MESH,
        )

    def whole_copy(source, target, send_sem, recv_sem, chunk):
        return pltpu.make_async_remote_copy(
            src_ref=source.at[chunk, 0:31],
            dst_ref=target.at[chunk, 0:31],
            send_sem=send_sem.at[chunk],
            recv_sem=recv_sem.at[chunk],
            device_id={"mem": other_core, "slab": me},
            device_id_type=MESH,
        )

    def half_copy(chunk, half, slab):
        return pltpu.make_async_remote_copy(
            src_ref=send_b.at[chunk, slab, half],
            dst_ref=recv_b.at[chunk, me, half],
            send_sem=half_sems.at[0, half, chunk],
            recv_sem=half_sems.at[1, half, chunk],
            device_id={"mem": mem, "slab": slab},
            device_id_type=MESH,
        )

    def whole_half(chunk, half):
        return pltpu.make_async_remote_copy(
            src_ref=send_b.at[chunk, 0:31, half],
            dst_ref=recv_b.at[chunk, 0:31, half],
            send_sem=half_sems.at[0, half, chunk],
            recv_sem=half_sems.at[1, half, chunk],
            device_id={"mem": other_core, "slab": me},
            device_id_type=MESH,
        )

    def forward_class(chunk):
        def second_step(b, inner):
            rows = pl.ds(pl.multiple_of(b * 16, 16), 16)
            values = [
                (work[chunk * SIZE + n, rows, 0:128], work[chunk * SIZE + n, rows, 128:256])
                for n in range(SIZE)
            ]
            for m, (re, im) in enumerate(short_transform(values, -1)):
                at = chunk * SIZE + m
                cos, sin = twist[0, at, 0:1, :], twist[1, at, 0:1, :]
                work[at, rows, 0:128] = re * cos + im * sin
                work[at, rows, 128:256] = im * cos - re * sin
            return inner

        lax.fori_loop(0, 8, second_step, 0)

        def one_pair(p, inner):
            first = pl.multiple_of(chunk * SIZE + p * 2, 2)
            both = three_parts(work[pl.ds(first, 2)].reshape(256, 256))
            result = lax.dot_general(
                forward_flip[...], both, (((1,), (1,)), ((), ())), preferred_element_type=F32
            )
            rows = pl.ds(pl.multiple_of(p * 8, 8), 8)
            for part_at in range(2):
                piece = result[128 * part_at : 128 * part_at + 128]
                even, odd = interlaced(
                    piece[:, :128].reshape(16, 8, 128), piece[:, 128:].reshape(16, 8, 128)
                )
                for d in range(16):
                    send_a[chunk, 2 * d, part_at, rows, :] = even[d]
                    send_a[chunk, 2 * d + 1, part_at, rows, :] = odd[d]
            return inner

        lax.fori_loop(0, SIZE // 2, one_pair, 0, unroll=True)

    def forward_send(chunk):
        for offset in OFFSETS:
            send_copy(send_a, recv_a, send_a_sem, recv_a_sem, chunk, slab_at(offset)).start()
        recv_a[chunk, me] = send_a[chunk, me]

    load_twist.wait()
    load_flip.wait()
    forward_class(0)
    pl.semaphore_wait(barrier, len(OFFSETS) + 2)
    forward_send(0)

    def forward_later(chunk, carry):
        forward_class(chunk)
        forward_send(chunk)
        return carry

    lax.fori_loop(1, CLASSES, forward_later, 0)

    load_forward.wait()
    load_inverse.wait()
    load_spectrum.wait()

    def flip_spectrum(k, carry):
        piece = spec[pl.ds(k, 128, stride=32), :] * (1.0 / (4096.0 * 4096.0))
        turned[...] = piece.T
        for c in range(CLASSES):
            for b in range(4):
                spec_flip[k, pl.ds(ROWS * c + b, SIZE, stride=4), :] = turned[
                    pl.ds(32 * b + c, SIZE, stride=CLASSES), :
                ]
        return carry

    lax.fori_loop(0, 32, flip_spectrum, 0)

    def widen(b, carry):
        rows = pl.ds(pl.multiple_of(b * 16, 16), 16)
        wide[:, rows, :] = anom[:, rows, :].astype(F32)
        return carry

    lax.fori_loop(0, 8, widen, 0)

    def columns(chunk, carry):
        whole_copy(send_a, recv_a, send_a_sem, recv_a_sem, chunk).wait_recv()

        def down(q, inner):
            rows = pl.ds(pl.multiple_of(q * 8, 8), 8)
            values = [
                (recv_a[chunk, s, 0, rows, :], recv_a[chunk, s, 1, rows, :]) for s in range(32)
            ]
            values = twisted(short_transform(values, -1), -1)
            for k in range(32):
                column[k, rows, 0:128] = values[k][0]
                column[k, rows, 128:256] = values[k][1]
            return inner

        lax.fori_loop(0, ROWS // 8, down, 0)
        share = pl.ds(pl.multiple_of(chunk * ROWS, ROWS), ROWS)

        def across(g, inner):
            group = pl.ds(pl.multiple_of(g * 256 // ROWS, 256 // ROWS), 256 // ROWS)
            waves = jnp.dot(
                three_parts(column[group].reshape(256, 256)), forward[...],
                preferred_element_type=F32,
            )
            scale = spec_flip[group, share, :].reshape(256, 128)
            waves = jnp.concatenate([waves[:, :128] * scale, waves[:, 128:] * scale], axis=1)
            back = jnp.dot(three_parts(waves), inverse[...], preferred_element_type=F32)
            column[group] = back.reshape(256 // ROWS, ROWS, 256)
            return inner

        lax.fori_loop(0, ROWS // 8, across, 0)

        def up(q, inner):
            rows = pl.ds(pl.multiple_of(q * 8, 8), 8)
            values = [(column[k, rows, 0:128], column[k, rows, 128:256]) for k in range(32)]
            values = short_transform(twisted(values, 1), 1)
            for s in range(32):
                staged[s, 0, rows, :] = values[s][0]
                staged[s, 1, rows, :] = values[s][1]
            return inner

        lax.fori_loop(0, ROWS // 8, up, 0)

        def pack(g, inner):
            for i in range(4):
                for part_at in range(2):
                    a, b = staged[4 * g + i, part_at, 0:8, :], staged[4 * g + i, part_at, 8:16, :]
                    send_b[chunk, 4 * g + i, 0, part_at] = jnp.where(left, a, pltpu.roll(b, 64, 1))
                    send_b[chunk, 4 * g + i, 1, part_at] = jnp.where(left, pltpu.roll(a, 64, 1), b)
            return inner

        lax.fori_loop(0, 8, pack, 0)

        @pl.when(chunk < CLASSES - DEFERRED)
        def _():
            for offset in OFFSETS:
                send_copy(send_b, recv_b, send_b_sem, recv_b_sem, chunk, slab_at(offset)).start()

        @pl.when(chunk >= CLASSES - DEFERRED)
        def _():
            for offset in OFFSETS:
                half_copy(chunk, 0, slab_at(offset)).start()

        recv_b[chunk, me] = send_b[chunk, me]
        return carry

    lax.fori_loop(0, CLASSES, columns, 0)

    def send_second(chunk, carry):
        for offset in OFFSETS:
            half_copy(chunk, 1, slab_at(offset)).start()
        return carry

    lax.fori_loop(CLASSES - DEFERRED, CLASSES, send_second, 0)

    def inverse_half(chunk, half):
        halves = []
        for part_at in range(2):
            even = jnp.stack([recv_b[chunk, 2 * d, half, part_at] for d in range(16)])
            odd = jnp.stack([recv_b[chunk, 2 * d + 1, half, part_at] for d in range(16)])
            a, b = interlaced(even, odd)
            halves.append((a.reshape(128, 128).T, b.reshape(128, 128).T))
        both = jnp.concatenate(
            [jnp.concatenate([halves[0][i], halves[1][i]], axis=1) for i in range(2)], axis=0
        )
        result = jnp.dot(three_parts(both), inverse[...], preferred_element_type=F32)
        rows = pl.ds(64 * half, 64)
        for i in range(2):
            for k in range(2):
                at = chunk * SIZE + 2 * k + i
                cos, sin = twist[0, at, 0:1, :], twist[1, at, 0:1, :]
                first = 128 * i + 64 * k
                re, im = result[first : first + 64, :128], result[first : first + 64, 128:]
                work[at, rows, 0:128] = re * cos - im * sin
                work[at, rows, 128:256] = re * sin + im * cos

    def inverse_rows(chunk, carry):
        whole_copy(send_b, recv_b, send_b_sem, recv_b_sem, chunk).wait_recv()
        inverse_half(chunk, 0)
        inverse_half(chunk, 1)
        return carry

    lax.fori_loop(0, CLASSES - DEFERRED, inverse_rows, 0)

    def member_sum(b):
        rows = pl.ds(pl.multiple_of(b * 8, 8), 8)
        values = [
            (work[place_of(a), rows, 0:128], work[place_of(a), rows, 128:256]) for a in range(32)
        ]
        for a, (re, im) in enumerate(short_transform(values, 1)):
            lanes = slice(128 * a, 128 * a + 128)
            part[b, :, lanes] = wide[0, rows, lanes] * re + wide[1, rows, lanes] * im

    def to_core(t):
        return pltpu.make_async_remote_copy(
            src_ref=part.at[2 * t + 1 - core],
            dst_ref=recv_part.at[t],
            send_sem=part_sems.at[0, t],
            recv_sem=part_sems.at[1, t],
            device_id={"mem": other_core, "slab": me},
            device_id_type=MESH,
        )

    def to_chip(t):
        return pltpu.make_async_remote_copy(
            src_ref=pair.at[t],
            dst_ref=recv_pair.at[t],
            send_sem=pair_sems.at[0, t],
            recv_sem=pair_sems.at[1, t],
            device_id={"mem": other_chip, "slab": me},
            device_id_type=MESH,
        )

    def block_rows(block):
        return pl.ds(pl.multiple_of(block * 8, 8), 8)

    def finished(t):
        rows = block_rows(2 * t + core)
        return pltpu.make_async_remote_copy(
            src_ref=out.at[rows, :],
            dst_ref=out.at[rows, :],
            send_sem=total_sems.at[0, t],
            recv_sem=total_sems.at[1, t],
            device_id={"mem": other_core, "slab": me},
            device_id_type=MESH,
        )

    def pass_on(t):
        to_core(t).wait_recv()
        pair[t] = part[2 * t + core] + recv_part[t]
        to_chip(t).start()

    def sum_and_send(t, carry):
        member_sum(2 * t + 1 - core)
        to_core(t).start()
        member_sum(2 * t + core)

        @pl.when(t % 4 >= 1)
        def _():
            pass_on(t - 1)

        return carry

    for half in range(2):

        def last_rows(chunk, carry, half=half):
            whole_half(chunk, half).wait_recv()
            inverse_half(chunk, half)
            return carry

        lax.fori_loop(CLASSES - DEFERRED, CLASSES, last_rows, 0)
        lax.fori_loop(4 * half, 4 * half + 4, sum_and_send, 0)
        pass_on(4 * half + 3)

    def finish(t, carry):
        to_chip(t).wait_recv()
        out[block_rows(2 * t + core), :] = pair[t] + recv_pair[t]
        finished(t).start()
        return carry

    lax.fori_loop(0, 8, finish, 0)

    def drain_slab(t, carry):
        whole_copy(send_a, recv_a, send_a_sem, recv_a_sem, t).wait_send()
        return carry

    lax.fori_loop(0, CLASSES, drain_slab, 0)

    def drain_back(t, carry):
        whole_copy(send_b, recv_b, send_b_sem, recv_b_sem, t).wait_send()
        return carry

    lax.fori_loop(0, CLASSES - DEFERRED, drain_back, 0)

    def drain_half(t, carry):
        whole_half(t, 0).wait_send()
        whole_half(t, 1).wait_send()
        return carry

    lax.fori_loop(CLASSES - DEFERRED, CLASSES, drain_half, 0)

    def drain(t, carry):
        to_core(t).wait_send()
        to_chip(t).wait_send()
        finished(t).wait_send()
        finished(t).wait_recv()
        return carry

    lax.fori_loop(0, 8, drain, 0)


def per_device(anomalies, increment, spectrum):
    tables, twist = constant_tables()
    vmem = pl.BlockSpec(memory_space=pltpu.VMEM)
    anywhere = pl.BlockSpec(memory_space=pl.ANY)
    dma = pltpu.SemaphoreType.DMA
    return pl.pallas_call(
        kernel,
        out_shape=pltpu.VMEM((128, 4096), F32),
        in_specs=[anywhere] * 7,
        out_specs=vmem,
        scratch_shapes=[
            pltpu.VMEM((256, 768), BF16),
            pltpu.VMEM((768, 256), BF16),
            pltpu.VMEM((768, 256), BF16),
            pltpu.VMEM((2, 32, 8, 128), F32),
            pltpu.VMEM((2, 128, 4096), BF16),
            pltpu.VMEM((2, 128, 4096), F32),
            pltpu.VMEM((128, 4096), F32),
            pltpu.VMEM((4096, 128), F32),
            pltpu.VMEM((128, 128), F32),
            pltpu.VMEM((32, 128, 128), F32),
            pltpu.VMEM((32, 128, 256), F32),
            pltpu.VMEM((CLASSES, 32, 2, ROWS, 128), F32),
            pltpu.VMEM((CLASSES, 32, 2, ROWS, 128), F32),
            pltpu.VMEM((32, ROWS, 256), F32),
            pltpu.VMEM((32, 2, ROWS, 128), F32),
            pltpu.VMEM((CLASSES, 32, 2, 2, 8, 128), F32),
            pltpu.VMEM((CLASSES, 32, 2, 2, 8, 128), F32),
            pltpu.VMEM((16, 8, 4096), F32),
            pltpu.VMEM((8, 8, 4096), F32),
            pltpu.VMEM((8, 8, 4096), F32),
            pltpu.VMEM((8, 8, 4096), F32),
            dma((21,)),
            dma((CLASSES,)), dma((CLASSES,)), dma((CLASSES,)), dma((CLASSES,)),
            dma((2, 2, CLASSES)),
            dma((2, 8)), dma((2, 8)), dma((2, 8)),
        ],
        compiler_params=pltpu.CompilerParams(
            collective_id=0, has_side_effects=True, vmem_limit_bytes=58 * 2**20
        ),
        name="covariance",
    )(anomalies, increment, spectrum, *[jnp.asarray(t) for t in tables], jnp.asarray(twist))


def solution(mesh):
    placed = (P("mem", "slab", None), P("slab", None), P(None, "slab"))
    return jax.shard_map(
        per_device, mesh=mesh, in_specs=placed, out_specs=P("slab", None), check_vma=False
    )
```

```python
import math

import jax
import jax.numpy as jnp
import numpy as np
from jax import lax
from jax.experimental import pallas as pl
from jax.experimental.pallas import tpu as pltpu
from jax.sharding import PartitionSpec as P

MESH = pl.DeviceIdType.MESH
F32 = jnp.float32
BF16 = jnp.bfloat16
ROOT_HALF = math.sqrt(0.5)
CLASSES = 8
SIZE = 32 // CLASSES
DEFERRED = 8
ROWS = 4 * SIZE

ROUNDS = (
    (2, 2), (1, 1), (3, 3), (0, 0), (1, 3), (3, 1), (0, 2), (2, 0),
    (1, 0), (3, 2), (1, 2), (3, 0), (0, 1), (2, 3), (2, 1), (0, 3),
)
OFFSETS = tuple(
    offset
    for a, b in ROUNDS
    for offset in ((a, b, 1), ((a + 2) % 4, (b + 2) % 4, 0))
    if offset != (0, 0, 0)
)


def constant_tables():
    index = np.arange(128)
    angle = 2.0 * np.pi / 128 * (np.outer(index, index) % 128)
    cos, sin = np.cos(angle), np.sin(angle)
    tables = []
    for sign in (-1.0, 1.0):
        block = np.block([[cos, sign * sin], [-sign * sin, cos]])
        if sign < 0:
            flipped = block.T
            high = flipped.astype(BF16)
            low = (flipped - high.astype(np.float64)).astype(BF16)
            tables.append(np.concatenate([high, high, low], axis=1))
        high = block.astype(BF16)
        low = (block - high.astype(np.float64)).astype(BF16)
        tables.append(np.concatenate([high, high, low], axis=0))
    order = np.arange(32) % SIZE * CLASSES + np.arange(32) // SIZE
    twist = 2.0 * np.pi / 4096 * np.outer(order, index)
    twist = np.stack([np.cos(twist), np.sin(twist)]).astype(np.float32)
    twist = np.broadcast_to(twist[:, :, None, :], (2, 32, 8, 128)).copy()
    return tables, twist


def short_transform(values, sign):
    count = len(values)
    if count == 1:
        return values
    even = short_transform(values[0::2], sign)
    odd = short_transform(values[1::2], sign)
    first, second = [], []
    for k in range(count // 2):
        (er, ei), (xr, xi) = even[k], odd[k]
        if k == 0:
            tr, ti = xr, xi
        elif 4 * k == count:
            if sign > 0:
                first.append((er - xi, ei + xr))
                second.append((er + xi, ei - xr))
            else:
                first.append((er + xi, ei - xr))
                second.append((er - xi, ei + xr))
            continue
        elif 8 * k == count:
            tr = (xr - sign * xi if sign > 0 else xr + xi) * ROOT_HALF
            ti = (xi + xr if sign > 0 else xi - xr) * ROOT_HALF
        elif 8 * k == 3 * count:
            tr = (xr + xi if sign > 0 else xr - xi) * -ROOT_HALF
            ti = (xr - xi if sign > 0 else -xr - xi) * ROOT_HALF
        else:
            cos = math.cos(2.0 * math.pi * k / count)
            sin = sign * math.sin(2.0 * math.pi * k / count)
            tr = xr * cos - xi * sin
            ti = xr * sin + xi * cos
        first.append((er + tr, ei + ti))
        second.append((er - tr, ei - ti))
    return first + second


def place_of(wave):
    return SIZE * (wave % CLASSES) + wave // CLASSES


def three_parts(x):
    high = x.astype(BF16)
    low = (x - high.astype(F32)).astype(BF16)
    return jnp.concatenate([high, low, high], axis=1)


def kernel(
    anomalies, increment, spectrum, flip_table, forward_table, inverse_table, twist_table, out,
    forward_flip, forward, inverse, twist,
    anom, held, given, incr, spec, turned, spec_flip, work, send_a, recv_a,
    column, staged, send_b, recv_b, part, recv_part, pair, recv_pair,
    load_sem, swap_sems, sems_a, sems_b, own_sems, part_sems, pair_sems, total_sems,
):
    me = lax.axis_index("slab")
    mem = lax.axis_index("mem")
    z, y, x = me // 8, (me // 2) % 4, me % 2
    core = mem % 2
    other_core = (mem // 2) * 2 + (1 - core)
    other_chip = (1 - mem // 2) * 2 + core
    moved = (x + core + 1) % 2

    def slab_at(offset):
        dz, dy, dx = offset
        return ((z + dz) % 4) * 8 + ((y + dy) % 4) * 2 + (x + dx) % 2

    barrier = pltpu.get_barrier_semaphore()
    for offset in OFFSETS:
        for mate in (mem, other_chip):
            pl.semaphore_signal(
                barrier,
                inc=1,
                device_id={"mem": mate, "slab": slab_at(offset)},
                device_id_type=MESH,
            )
    for mate in (other_core, other_chip):
        pl.semaphore_signal(
            barrier, inc=1, device_id={"mem": mate, "slab": me}, device_id_type=MESH
        )

    def load_anomalies(b):
        rows = pl.ds(pl.multiple_of(b * 16, 16), 16)
        return pltpu.make_async_copy(anomalies.at[:, rows, :], anom.at[:, rows, :], load_sem.at[b])

    def load_increment(b):
        rows = pl.ds(pl.multiple_of(b * 16, 16), 16)
        return pltpu.make_async_copy(increment.at[rows, :], incr.at[rows, :], load_sem.at[8 + b])

    def start_loads(b, carry):
        load_anomalies(b).start()
        load_increment(b).start()
        return carry

    load_twist = pltpu.make_async_copy(twist_table, twist, load_sem.at[17])
    load_flip = pltpu.make_async_copy(flip_table, forward_flip, load_sem.at[18])
    load_forward = pltpu.make_async_copy(forward_table, forward, load_sem.at[19])
    load_inverse = pltpu.make_async_copy(inverse_table, inverse, load_sem.at[20])
    load_spectrum = pltpu.make_async_copy(spectrum, spec, load_sem.at[16])
    lax.fori_loop(0, 8, start_loads, 0)
    for copy in (load_twist, load_flip, load_forward, load_inverse, load_spectrum):
        copy.start()

    sub = lax.broadcasted_iota(jnp.int32, (16, 8, 128), 1)
    lower = sub < 4
    left = lax.broadcasted_iota(jnp.int32, (8, 128), 1) < 64

    def interlaced(a, b):
        even = jnp.where(lower, a, pltpu.roll(b, 4, 1))
        odd = jnp.where(lower, pltpu.roll(a, 4, 1), b)
        return even, odd

    def twisted(values, sign):
        result = [values[0]]
        for k in range(1, 32):
            re, im = values[k]
            cos, sin = twist[0, place_of(k)], twist[1, place_of(k)]
            if sign > 0:
                result.append((re * cos - im * sin, re * sin + im * cos))
            else:
                result.append((re * cos + im * sin, im * cos - re * sin))
        return result

    def swap(b):
        rows = pl.ds(pl.multiple_of(b * 16, 16), 16)
        return pltpu.make_async_remote_copy(
            src_ref=given.at[:, rows, :],
            dst_ref=held.at[:, rows, :],
            send_sem=swap_sems.at[0, b],
            recv_sem=swap_sems.at[1, b],
            device_id={"mem": other_chip, "slab": me},
            device_id_type=MESH,
        )

    def widen(b, carry):
        load_anomalies(b).wait()
        load_increment(b).wait()
        rows = pl.ds(pl.multiple_of(b * 16, 16), 16)

        @pl.when((moved == 1) & (b < 4))
        def _():
            given[:, pl.ds(pl.multiple_of((b % 4) * 16, 16), 16), :] = anom[:, rows, :].astype(F32)

        @pl.when((moved == 0) | (b >= 4))
        def _():
            held[:, rows, :] = anom[:, rows, :].astype(F32)

        return carry

    def first_step(b, carry):
        rows = pl.ds(pl.multiple_of(b * 16, 16), 16)
        for n in range(SIZE):
            inputs = []
            for p in range(CLASSES):
                lanes = slice(128 * (n + SIZE * p), 128 * (n + SIZE * p) + 128)
                step = incr[rows, lanes]
                inputs.append(
                    (held[0, rows, lanes] * step, held[1, rows, lanes] * step)
                )
            for c, (re, im) in enumerate(short_transform(inputs, -1)):
                if c * n:
                    cos = math.cos(2.0 * math.pi * c * n / 32)
                    sin = -math.sin(2.0 * math.pi * c * n / 32)
                    re, im = re * cos - im * sin, re * sin + im * cos
                work[SIZE * c + n, rows, 0:128] = re
                work[SIZE * c + n, rows, 128:256] = im
        return carry

    lax.fori_loop(4, 8, widen, 0)
    lax.fori_loop(4, 8, first_step, 0)
    lax.fori_loop(0, 4, widen, 0)

    def mem_at(other):
        return ((mem // 2 + other) % 2) * 2 + core

    def half_copy(source, target, sems, chunk, half, slab, mate):
        return pltpu.make_async_remote_copy(
            src_ref=source.at[chunk, slab, half],
            dst_ref=target.at[chunk, me, half],
            send_sem=sems.at[0, half, chunk],
            recv_sem=sems.at[1, half, chunk],
            device_id={"mem": mate, "slab": slab},
            device_id_type=MESH,
        )

    def all_copies(source, target, sems, chunk, half):
        return pltpu.make_async_remote_copy(
            src_ref=source.at[chunk, 0:31, half],
            dst_ref=target.at[chunk, 0:31, half],
            send_sem=sems.at[0, half, chunk],
            recv_sem=sems.at[1, half, chunk],
            device_id={"mem": other_chip, "slab": me},
            device_id_type=MESH,
        )

    def own_copy(source, target, way, chunk):
        return pltpu.make_async_remote_copy(
            src_ref=source.at[chunk, me, 1],
            dst_ref=target.at[chunk, me, 1],
            send_sem=own_sems.at[way, 0, chunk],
            recv_sem=own_sems.at[way, 1, chunk],
            device_id={"mem": other_chip, "slab": me},
            device_id_type=MESH,
        )

    def keep_own(source, target, way, chunk, half):
        if half == 0:
            target[chunk, me, 0] = source[chunk, me, 0]
            return

        @pl.when(moved == 1)
        def _():
            own_copy(source, target, way, chunk).start()

        @pl.when(moved == 0)
        def _():
            target[chunk, me, 1] = source[chunk, me, 1]

    def arrived(source, target, sems, way, chunk, half):
        all_copies(source, target, sems, chunk, half).wait_recv()
        if half == 1:

            @pl.when(moved == 1)
            def _():
                own_copy(source, target, way, chunk).wait_recv()

    def send_forward(chunk, half):
        for offset in OFFSETS:
            mate = mem_at(offset[2] + moved * half)
            half_copy(send_a, recv_a, sems_a, chunk, half, slab_at(offset), mate).start()
        keep_own(send_a, recv_a, 0, chunk, half)

    def send_back(chunk, half):
        for offset in OFFSETS:
            mate = mem_at(offset[2] + ((moved + offset[2]) % 2) * half)
            half_copy(send_b, recv_b, sems_b, chunk, half, slab_at(offset), mate).start()
        keep_own(send_b, recv_b, 1, chunk, half)

    def forward_class(chunk, half):
        def second_step(b, inner):
            rows = pl.ds(pl.multiple_of(64 * half + b * 16, 16), 16)
            values = [
                (work[chunk * SIZE + n, rows, 0:128], work[chunk * SIZE + n, rows, 128:256])
                for n in range(SIZE)
            ]
            for m, (re, im) in enumerate(short_transform(values, -1)):
                at = chunk * SIZE + m
                cos, sin = twist[0, at, 0:1, :], twist[1, at, 0:1, :]
                work[at, rows, 0:128] = re * cos + im * sin
                work[at, rows, 128:256] = im * cos - re * sin
            return inner

        lax.fori_loop(0, 4, second_step, 0)
        rows = pl.ds(64 * half, 64)
        both = three_parts(
            jnp.concatenate([work[chunk * SIZE + m, rows, :] for m in (0, 2, 1, 3)], axis=0)
        )
        result = lax.dot_general(
            forward_flip[...], both, (((1,), (1,)), ((), ())), preferred_element_type=F32
        )
        for part_at in range(2):
            piece = result[128 * part_at : 128 * part_at + 128]
            even, odd = interlaced(
                piece[:, :128].reshape(16, 8, 128), piece[:, 128:].reshape(16, 8, 128)
            )
            for d in range(16):
                send_a[chunk, 2 * d, half, part_at] = even[d]
                send_a[chunk, 2 * d + 1, half, part_at] = odd[d]

    load_twist.wait()
    load_flip.wait()
    forward_class(0, 1)
    pl.semaphore_wait(barrier, 2 * len(OFFSETS) + 2)

    @pl.when(moved == 1)
    def _():
        for b in range(4):
            swap(b).start()

    send_forward(0, 1)

    def forward_second(chunk, carry):
        forward_class(chunk, 1)
        send_forward(chunk, 1)
        return carry

    lax.fori_loop(1, CLASSES, forward_second, 0)

    load_forward.wait()
    load_inverse.wait()
    load_spectrum.wait()

    def flip_spectrum(k, carry):
        piece = spec[pl.ds(k, 128, stride=32), :] * (1.0 / (4096.0 * 4096.0))
        turned[...] = piece.T
        for c in range(CLASSES):
            for b in range(4):
                spec_flip[k, pl.ds(ROWS * c + b, SIZE, stride=4), :] = turned[
                    pl.ds(32 * b + c, SIZE, stride=CLASSES), :
                ]
        return carry

    lax.fori_loop(0, 32, flip_spectrum, 0)

    def late_step(b, carry):
        @pl.when(moved == 1)
        def _():
            swap(b).wait_recv()

        return first_step(b, carry)

    lax.fori_loop(0, 4, late_step, 0)

    def forward_first(chunk, carry):
        forward_class(chunk, 0)
        send_forward(chunk, 0)
        return carry

    lax.fori_loop(0, CLASSES, forward_first, 0)

    def columns(chunk, carry):
        arrived(send_a, recv_a, sems_a, 0, chunk, 1)
        arrived(send_a, recv_a, sems_a, 0, chunk, 0)

        def unpack(g, inner):
            for i in range(4):
                for part_at in range(2):
                    a = recv_a[chunk, 4 * g + i, 0, part_at]
                    b = recv_a[chunk, 4 * g + i, 1, part_at]
                    staged[4 * g + i, part_at, 0:8, :] = jnp.where(left, a, pltpu.roll(b, 64, 1))
                    staged[4 * g + i, part_at, 8:16, :] = jnp.where(left, pltpu.roll(a, 64, 1), b)
            return inner

        lax.fori_loop(0, 8, unpack, 0)

        def down(q, inner):
            rows = pl.ds(pl.multiple_of(q * 8, 8), 8)
            values = [
                (staged[s, 0, rows, :], staged[s, 1, rows, :]) for s in range(32)
            ]
            values = twisted(short_transform(values, -1), -1)
            for k in range(32):
                column[k, rows, 0:128] = values[k][0]
                column[k, rows, 128:256] = values[k][1]
            return inner

        lax.fori_loop(0, ROWS // 8, down, 0)
        share = pl.ds(pl.multiple_of(chunk * ROWS, ROWS), ROWS)

        def across(g, inner):
            group = pl.ds(pl.multiple_of(g * 256 // ROWS, 256 // ROWS), 256 // ROWS)
            waves = jnp.dot(
                three_parts(column[group].reshape(256, 256)), forward[...],
                preferred_element_type=F32,
            )
            scale = spec_flip[group, share, :].reshape(256, 128)
            waves = jnp.concatenate([waves[:, :128] * scale, waves[:, 128:] * scale], axis=1)
            back = jnp.dot(three_parts(waves), inverse[...], preferred_element_type=F32)
            column[group] = back.reshape(256 // ROWS, ROWS, 256)
            return inner

        lax.fori_loop(0, ROWS // 8, across, 0)

        def up(q, inner):
            rows = pl.ds(pl.multiple_of(q * 8, 8), 8)
            values = [(column[k, rows, 0:128], column[k, rows, 128:256]) for k in range(32)]
            values = short_transform(twisted(values, 1), 1)
            for s in range(32):
                staged[s, 0, rows, :] = values[s][0]
                staged[s, 1, rows, :] = values[s][1]
            return inner

        lax.fori_loop(0, ROWS // 8, up, 0)

        def pack(g, inner):
            for i in range(4):
                for part_at in range(2):
                    a, b = staged[4 * g + i, part_at, 0:8, :], staged[4 * g + i, part_at, 8:16, :]
                    send_b[chunk, 4 * g + i, 0, part_at] = jnp.where(left, a, pltpu.roll(b, 64, 1))
                    send_b[chunk, 4 * g + i, 1, part_at] = jnp.where(left, pltpu.roll(a, 64, 1), b)
            return inner

        lax.fori_loop(0, 8, pack, 0)

        send_back(chunk, 1)

        @pl.when(chunk < CLASSES - DEFERRED)
        def _():
            send_back(chunk, 0)

        return carry

    lax.fori_loop(0, CLASSES, columns, 0)

    def send_second(chunk, carry):
        send_back(chunk, 0)
        return carry

    lax.fori_loop(CLASSES - DEFERRED, CLASSES, send_second, 0)

    def inverse_half(chunk, half):
        halves = []
        for part_at in range(2):
            even = jnp.stack([recv_b[chunk, 2 * d, half, part_at] for d in range(16)])
            odd = jnp.stack([recv_b[chunk, 2 * d + 1, half, part_at] for d in range(16)])
            a, b = interlaced(even, odd)
            halves.append((a.reshape(128, 128).T, b.reshape(128, 128).T))
        both = jnp.concatenate(
            [jnp.concatenate([halves[0][i], halves[1][i]], axis=1) for i in range(2)], axis=0
        )
        result = jnp.dot(three_parts(both), inverse[...], preferred_element_type=F32)
        rows = pl.ds(64 * half, 64)
        for i in range(2):
            for k in range(2):
                at = chunk * SIZE + 2 * k + i
                cos, sin = twist[0, at, 0:1, :], twist[1, at, 0:1, :]
                first = 128 * i + 64 * k
                re, im = result[first : first + 64, :128], result[first : first + 64, 128:]
                work[at, rows, 0:128] = re * cos - im * sin
                work[at, rows, 128:256] = re * sin + im * cos

    def member_sum(b):
        rows = pl.ds(pl.multiple_of(b * 8, 8), 8)
        values = [
            (work[place_of(a), rows, 0:128], work[place_of(a), rows, 128:256]) for a in range(32)
        ]
        for a, (re, im) in enumerate(short_transform(values, 1)):
            lanes = slice(128 * a, 128 * a + 128)
            part[b, :, lanes] = held[0, rows, lanes] * re + held[1, rows, lanes] * im

    def to_core(t):
        return pltpu.make_async_remote_copy(
            src_ref=part.at[2 * t + 1 - core],
            dst_ref=recv_part.at[t],
            send_sem=part_sems.at[0, t],
            recv_sem=part_sems.at[1, t],
            device_id={"mem": other_core, "slab": me},
            device_id_type=MESH,
        )

    def to_chip(t):
        return pltpu.make_async_remote_copy(
            src_ref=pair.at[t],
            dst_ref=recv_pair.at[t],
            send_sem=pair_sems.at[0, t],
            recv_sem=pair_sems.at[1, t],
            device_id={"mem": other_chip, "slab": me},
            device_id_type=MESH,
        )

    def block_rows(block):
        return pl.ds(pl.multiple_of(block * 8, 8), 8)

    def finished(t):
        rows = block_rows(2 * t + core)
        return pltpu.make_async_remote_copy(
            src_ref=out.at[rows, :],
            dst_ref=out.at[rows, :],
            send_sem=total_sems.at[0, t],
            recv_sem=total_sems.at[1, t],
            device_id={"mem": other_core, "slab": me},
            device_id_type=MESH,
        )

    def pass_on(t):
        to_core(t).wait_recv()
        pair[t] = part[2 * t + core] + recv_part[t]
        to_chip(t).start()

    def sum_and_send(t, carry):
        member_sum(2 * t + 1 - core)
        to_core(t).start()
        member_sum(2 * t + core)

        @pl.when(t % 4 >= 1)
        def _():
            pass_on(t - 1)

        return carry

    for half in (1, 0):

        def last_rows(chunk, carry, half=half):
            arrived(send_b, recv_b, sems_b, 1, chunk, half)
            inverse_half(chunk, half)
            return carry

        lax.fori_loop(0, CLASSES, last_rows, 0)
        lax.fori_loop(4 * half, 4 * half + 4, sum_and_send, 0)
        pass_on(4 * half + 3)

    def finish(t, carry):
        to_chip(t).wait_recv()
        out[block_rows(2 * t + core), :] = pair[t] + recv_pair[t]
        finished(t).start()
        return carry

    lax.fori_loop(0, 8, finish, 0)

    def drain_slab(t, carry):
        for half in range(2):
            all_copies(send_a, recv_a, sems_a, t, half).wait_send()
            all_copies(send_b, recv_b, sems_b, t, half).wait_send()

        @pl.when(moved == 1)
        def _():
            own_copy(send_a, recv_a, 0, t).wait_send()
            own_copy(send_b, recv_b, 1, t).wait_send()

        return carry

    lax.fori_loop(0, CLASSES, drain_slab, 0)

    @pl.when(moved == 1)
    def _():
        for b in range(4):
            swap(b).wait_send()

    def drain(t, carry):
        to_core(t).wait_send()
        to_chip(t).wait_send()
        finished(t).wait_send()
        finished(t).wait_recv()
        return carry

    lax.fori_loop(0, 8, drain, 0)


def per_device(anomalies, increment, spectrum):
    tables, twist = constant_tables()
    vmem = pl.BlockSpec(memory_space=pltpu.VMEM)
    anywhere = pl.BlockSpec(memory_space=pl.ANY)
    dma = pltpu.SemaphoreType.DMA
    return pl.pallas_call(
        kernel,
        out_shape=pltpu.VMEM((128, 4096), F32),
        in_specs=[anywhere] * 7,
        out_specs=vmem,
        scratch_shapes=[
            pltpu.VMEM((256, 768), BF16),
            pltpu.VMEM((768, 256), BF16),
            pltpu.VMEM((768, 256), BF16),
            pltpu.VMEM((2, 32, 8, 128), F32),
            pltpu.VMEM((2, 128, 4096), BF16),
            pltpu.VMEM((2, 128, 4096), F32),
            pltpu.VMEM((2, 64, 4096), F32),
            pltpu.VMEM((128, 4096), F32),
            pltpu.VMEM((4096, 128), F32),
            pltpu.VMEM((128, 128), F32),
            pltpu.VMEM((32, 128, 128), F32),
            pltpu.VMEM((32, 128, 256), F32),
            pltpu.VMEM((CLASSES, 32, 2, 2, 8, 128), F32),
            pltpu.VMEM((CLASSES, 32, 2, 2, 8, 128), F32),
            pltpu.VMEM((32, ROWS, 256), F32),
            pltpu.VMEM((32, 2, ROWS, 128), F32),
            pltpu.VMEM((CLASSES, 32, 2, 2, 8, 128), F32),
            pltpu.VMEM((CLASSES, 32, 2, 2, 8, 128), F32),
            pltpu.VMEM((16, 8, 4096), F32),
            pltpu.VMEM((8, 8, 4096), F32),
            pltpu.VMEM((8, 8, 4096), F32),
            pltpu.VMEM((8, 8, 4096), F32),
            dma((21,)),
            dma((2, 4)),
            dma((2, 2, CLASSES)), dma((2, 2, CLASSES)), dma((2, 2, CLASSES)),
            dma((2, 8)), dma((2, 8)), dma((2, 8)),
        ],
        compiler_params=pltpu.CompilerParams(
            collective_id=0, has_side_effects=True, vmem_limit_bytes=58 * 2**20
        ),
        name="covariance",
    )(anomalies, increment, spectrum, *[jnp.asarray(t) for t in tables], jnp.asarray(twist))


def solution(mesh):
    placed = (P("mem", "slab", None), P("slab", None), P(None, "slab"))
    return jax.shard_map(
        per_device, mesh=mesh, in_specs=placed, out_specs=P("slab", None), check_vma=False
    )
```

```python
import math

import jax
import jax.numpy as jnp
import numpy as np
from jax import lax
from jax.experimental import pallas as pl
from jax.experimental.pallas import tpu as pltpu
from jax.sharding import PartitionSpec as P

MESH = pl.DeviceIdType.MESH
F32 = jnp.float32
BF16 = jnp.bfloat16
ROOT_HALF = math.sqrt(0.5)
CLASSES = 8
SIZE = 32 // CLASSES
DEFERRED = 8
ROWS = 4 * SIZE

ROUNDS = (
    (2, 2), (1, 1), (3, 3), (0, 0), (1, 3), (3, 1), (0, 2), (2, 0),
    (1, 0), (3, 2), (1, 2), (3, 0), (0, 1), (2, 3), (2, 1), (0, 3),
)
OFFSETS = tuple(
    offset
    for a, b in ROUNDS
    for offset in ((a, b, 1), ((a + 2) % 4, (b + 2) % 4, 0))
    if offset != (0, 0, 0)
)


def constant_tables():
    index = np.arange(128)
    angle = 2.0 * np.pi / 128 * (np.outer(index, index) % 128)
    cos, sin = np.cos(angle), np.sin(angle)
    tables = []
    for sign in (-1.0, 1.0):
        block = np.block([[cos, sign * sin], [-sign * sin, cos]])
        if sign < 0:
            flipped = block.T
            high = flipped.astype(BF16)
            low = (flipped - high.astype(np.float64)).astype(BF16)
            tables.append(np.concatenate([high, high, low], axis=1))
        high = block.astype(BF16)
        low = (block - high.astype(np.float64)).astype(BF16)
        tables.append(np.concatenate([high, high, low], axis=0))
    order = np.arange(32) % SIZE * CLASSES + np.arange(32) // SIZE
    twist = 2.0 * np.pi / 4096 * np.outer(order, index)
    twist = np.stack([np.cos(twist), np.sin(twist)]).astype(np.float32)
    twist = np.broadcast_to(twist[:, :, None, :], (2, 32, 8, 128)).copy()
    return tables, twist


def short_transform(values, sign):
    count = len(values)
    if count == 1:
        return values
    even = short_transform(values[0::2], sign)
    odd = short_transform(values[1::2], sign)
    first, second = [], []
    for k in range(count // 2):
        (er, ei), (xr, xi) = even[k], odd[k]
        if k == 0:
            tr, ti = xr, xi
        elif 4 * k == count:
            if sign > 0:
                first.append((er - xi, ei + xr))
                second.append((er + xi, ei - xr))
            else:
                first.append((er + xi, ei - xr))
                second.append((er - xi, ei + xr))
            continue
        elif 8 * k == count:
            tr = (xr - sign * xi if sign > 0 else xr + xi) * ROOT_HALF
            ti = (xi + xr if sign > 0 else xi - xr) * ROOT_HALF
        elif 8 * k == 3 * count:
            tr = (xr + xi if sign > 0 else xr - xi) * -ROOT_HALF
            ti = (xr - xi if sign > 0 else -xr - xi) * ROOT_HALF
        else:
            cos = math.cos(2.0 * math.pi * k / count)
            sin = sign * math.sin(2.0 * math.pi * k / count)
            tr = xr * cos - xi * sin
            ti = xr * sin + xi * cos
        first.append((er + tr, ei + ti))
        second.append((er - tr, ei - ti))
    return first + second


def place_of(wave):
    return SIZE * (wave % CLASSES) + wave // CLASSES


def three_parts(x):
    high = x.astype(BF16)
    low = (x - high.astype(F32)).astype(BF16)
    return jnp.concatenate([high, low, high], axis=1)


def kernel(
    anomalies, increment, spectrum, flip_table, forward_table, inverse_table, twist_table, out,
    forward_flip, forward, inverse, twist,
    anom, held, given, incr, spec, turned, spec_flip, work, send_a, recv_a,
    column, staged, send_b, recv_b, part, recv_part, pair, recv_pair,
    load_sem, swap_sems, sems_a, sems_b, own_sems, part_sems, pair_sems, total_sems,
):
    me = lax.axis_index("slab")
    mem = lax.axis_index("mem")
    z, y, x = me // 8, (me // 2) % 4, me % 2
    core = mem % 2
    other_core = (mem // 2) * 2 + (1 - core)
    other_chip = (1 - mem // 2) * 2 + core
    moved = (x + core + 1) % 2

    def slab_at(offset):
        dz, dy, dx = offset
        return ((z + dz) % 4) * 8 + ((y + dy) % 4) * 2 + (x + dx) % 2

    barrier = pltpu.get_barrier_semaphore()
    for offset in OFFSETS:
        for mate in (mem, other_chip):
            pl.semaphore_signal(
                barrier,
                inc=1,
                device_id={"mem": mate, "slab": slab_at(offset)},
                device_id_type=MESH,
            )
    for mate in (other_core, other_chip):
        pl.semaphore_signal(
            barrier, inc=1, device_id={"mem": mate, "slab": me}, device_id_type=MESH
        )

    def load_anomalies(b):
        rows = pl.ds(pl.multiple_of(b * 16, 16), 16)
        return pltpu.make_async_copy(anomalies.at[:, rows, :], anom.at[:, rows, :], load_sem.at[b])

    def load_increment(b):
        rows = pl.ds(pl.multiple_of(b * 16, 16), 16)
        return pltpu.make_async_copy(increment.at[rows, :], incr.at[rows, :], load_sem.at[8 + b])

    def start_loads(b, carry):
        load_anomalies(b).start()
        load_increment(b).start()
        return carry

    load_twist = pltpu.make_async_copy(twist_table, twist, load_sem.at[17])
    load_flip = pltpu.make_async_copy(flip_table, forward_flip, load_sem.at[18])
    load_forward = pltpu.make_async_copy(forward_table, forward, load_sem.at[19])
    load_inverse = pltpu.make_async_copy(inverse_table, inverse, load_sem.at[20])
    load_spectrum = pltpu.make_async_copy(spectrum, spec, load_sem.at[16])
    lax.fori_loop(0, 8, start_loads, 0)
    for copy in (load_twist, load_flip, load_forward, load_inverse, load_spectrum):
        copy.start()

    sub = lax.broadcasted_iota(jnp.int32, (16, 8, 128), 1)
    lower = sub < 4
    left = lax.broadcasted_iota(jnp.int32, (8, 128), 1) < 64

    def interlaced(a, b):
        even = jnp.where(lower, a, pltpu.roll(b, 4, 1))
        odd = jnp.where(lower, pltpu.roll(a, 4, 1), b)
        return even, odd

    def twisted(values, sign):
        result = [values[0]]
        for k in range(1, 32):
            re, im = values[k]
            cos, sin = twist[0, place_of(k)], twist[1, place_of(k)]
            if sign > 0:
                result.append((re * cos - im * sin, re * sin + im * cos))
            else:
                result.append((re * cos + im * sin, im * cos - re * sin))
        return result

    def swap(b):
        rows = pl.ds(pl.multiple_of(b * 16, 16), 16)
        return pltpu.make_async_remote_copy(
            src_ref=given.at[:, rows, :],
            dst_ref=held.at[:, rows, :],
            send_sem=swap_sems.at[0, b],
            recv_sem=swap_sems.at[1, b],
            device_id={"mem": other_chip, "slab": me},
            device_id_type=MESH,
        )

    def widen(b, carry):
        load_anomalies(b).wait()
        load_increment(b).wait()
        rows = pl.ds(pl.multiple_of(b * 16, 16), 16)

        @pl.when((moved == 1) & (b < 4))
        def _():
            given[:, pl.ds(pl.multiple_of((b % 4) * 16, 16), 16), :] = anom[:, rows, :].astype(F32)

        @pl.when((moved == 0) | (b >= 4))
        def _():
            held[:, rows, :] = anom[:, rows, :].astype(F32)

        return carry

    def first_step(b, carry):
        rows = pl.ds(pl.multiple_of(b * 16, 16), 16)
        for n in range(SIZE):
            inputs = []
            for p in range(CLASSES):
                lanes = slice(128 * (n + SIZE * p), 128 * (n + SIZE * p) + 128)
                step = incr[rows, lanes]
                inputs.append(
                    (held[0, rows, lanes] * step, held[1, rows, lanes] * step)
                )
            for c, (re, im) in enumerate(short_transform(inputs, -1)):
                if c * n:
                    cos = math.cos(2.0 * math.pi * c * n / 32)
                    sin = -math.sin(2.0 * math.pi * c * n / 32)
                    re, im = re * cos - im * sin, re * sin + im * cos
                work[SIZE * c + n, rows, 0:128] = re
                work[SIZE * c + n, rows, 128:256] = im
        return carry

    lax.fori_loop(4, 8, widen, 0)
    lax.fori_loop(4, 8, first_step, 0)
    lax.fori_loop(0, 4, widen, 0)

    def mem_at(other):
        return ((mem // 2 + other) % 2) * 2 + core

    def half_copy(source, target, sems, chunk, half, slab, mate):
        return pltpu.make_async_remote_copy(
            src_ref=source.at[chunk, slab, half],
            dst_ref=target.at[chunk, me, half],
            send_sem=sems.at[0, half, chunk],
            recv_sem=sems.at[1, half, chunk],
            device_id={"mem": mate, "slab": slab},
            device_id_type=MESH,
        )

    def all_copies(source, target, sems, chunk, half):
        return pltpu.make_async_remote_copy(
            src_ref=source.at[chunk, 0:31, half],
            dst_ref=target.at[chunk, 0:31, half],
            send_sem=sems.at[0, half, chunk],
            recv_sem=sems.at[1, half, chunk],
            device_id={"mem": other_chip, "slab": me},
            device_id_type=MESH,
        )

    def own_copy(source, target, way, chunk):
        return pltpu.make_async_remote_copy(
            src_ref=source.at[chunk, me, 1],
            dst_ref=target.at[chunk, me, 1],
            send_sem=own_sems.at[way, 0, chunk],
            recv_sem=own_sems.at[way, 1, chunk],
            device_id={"mem": other_chip, "slab": me},
            device_id_type=MESH,
        )

    def keep_own(source, target, way, chunk, half):
        if half == 0:
            target[chunk, me, 0] = source[chunk, me, 0]
            return

        @pl.when(moved == 1)
        def _():
            own_copy(source, target, way, chunk).start()

        @pl.when(moved == 0)
        def _():
            target[chunk, me, 1] = source[chunk, me, 1]

    def arrived(source, target, sems, way, chunk, half):
        all_copies(source, target, sems, chunk, half).wait_recv()
        if half == 1:

            @pl.when(moved == 1)
            def _():
                own_copy(source, target, way, chunk).wait_recv()

    def send_forward(chunk, half):
        for offset in OFFSETS:
            mate = mem_at(offset[2] + moved * half)
            half_copy(send_a, recv_a, sems_a, chunk, half, slab_at(offset), mate).start()
        keep_own(send_a, recv_a, 0, chunk, half)

    def send_back(chunk, half):
        for offset in OFFSETS:
            mate = mem_at(offset[2] + ((moved + offset[2]) % 2) * half)
            half_copy(send_b, recv_b, sems_b, chunk, half, slab_at(offset), mate).start()
        keep_own(send_b, recv_b, 1, chunk, half)

    def forward_class(chunk, half):
        def second_step(b, inner):
            rows = pl.ds(pl.multiple_of(64 * half + b * 16, 16), 16)
            values = [
                (work[chunk * SIZE + n, rows, 0:128], work[chunk * SIZE + n, rows, 128:256])
                for n in range(SIZE)
            ]
            for m, (re, im) in enumerate(short_transform(values, -1)):
                at = chunk * SIZE + m
                cos, sin = twist[0, at, 0:1, :], twist[1, at, 0:1, :]
                work[at, rows, 0:128] = re * cos + im * sin
                work[at, rows, 128:256] = im * cos - re * sin
            return inner

        lax.fori_loop(0, 4, second_step, 0)
        rows = pl.ds(64 * half, 64)
        both = three_parts(
            jnp.concatenate([work[chunk * SIZE + m, rows, :] for m in (0, 2, 1, 3)], axis=0)
        )
        result = lax.dot_general(
            forward_flip[...], both, (((1,), (1,)), ((), ())), preferred_element_type=F32
        )
        for part_at in range(2):
            piece = result[128 * part_at : 128 * part_at + 128]
            even, odd = interlaced(
                piece[:, :128].reshape(16, 8, 128), piece[:, 128:].reshape(16, 8, 128)
            )
            for d in range(16):
                send_a[chunk, 2 * d, half, part_at] = even[d]
                send_a[chunk, 2 * d + 1, half, part_at] = odd[d]

    load_twist.wait()
    load_flip.wait()
    forward_class(0, 1)
    pl.semaphore_wait(barrier, 2 * len(OFFSETS) + 2)

    @pl.when(moved == 1)
    def _():
        for b in range(4):
            swap(b).start()

    send_forward(0, 1)

    def forward_second(chunk, carry):
        forward_class(chunk, 1)
        send_forward(chunk, 1)
        return carry

    lax.fori_loop(1, CLASSES, forward_second, 0)

    load_forward.wait()
    load_inverse.wait()
    load_spectrum.wait()

    def flip_spectrum(k, carry):
        piece = spec[pl.ds(k, 128, stride=32), :] * (1.0 / (4096.0 * 4096.0))
        turned[...] = piece.T
        for c in range(CLASSES):
            for b in range(4):
                spec_flip[k, pl.ds(ROWS * c + b, SIZE, stride=4), :] = turned[
                    pl.ds(32 * b + c, SIZE, stride=CLASSES), :
                ]
        return carry

    lax.fori_loop(0, 32, flip_spectrum, 0)

    def late_step(b, carry):
        @pl.when(moved == 1)
        def _():
            swap(b).wait_recv()

        return first_step(b, carry)

    lax.fori_loop(0, 4, late_step, 0)

    def forward_first(chunk, carry):
        forward_class(chunk, 0)
        send_forward(chunk, 0)
        return carry

    lax.fori_loop(0, CLASSES, forward_first, 0)

    def columns(chunk, carry):
        arrived(send_a, recv_a, sems_a, 0, chunk, 1)
        arrived(send_a, recv_a, sems_a, 0, chunk, 0)

        def unpack(g, inner):
            for i in range(4):
                for part_at in range(2):
                    a = recv_a[chunk, 4 * g + i, 0, part_at]
                    b = recv_a[chunk, 4 * g + i, 1, part_at]
                    staged[4 * g + i, part_at, 0:8, :] = jnp.where(left, a, pltpu.roll(b, 64, 1))
                    staged[4 * g + i, part_at, 8:16, :] = jnp.where(left, pltpu.roll(a, 64, 1), b)
            return inner

        lax.fori_loop(0, 8, unpack, 0)

        def down(q, inner):
            rows = pl.ds(pl.multiple_of(q * 8, 8), 8)
            values = [
                (staged[s, 0, rows, :], staged[s, 1, rows, :]) for s in range(32)
            ]
            values = twisted(short_transform(values, -1), -1)
            for k in range(32):
                column[k, rows, 0:128] = values[k][0]
                column[k, rows, 128:256] = values[k][1]
            return inner

        lax.fori_loop(0, ROWS // 8, down, 0)
        share = pl.ds(pl.multiple_of(chunk * ROWS, ROWS), ROWS)

        def across(g, inner):
            group = pl.ds(pl.multiple_of(g * 256 // ROWS, 256 // ROWS), 256 // ROWS)
            waves = jnp.dot(
                three_parts(column[group].reshape(256, 256)), forward[...],
                preferred_element_type=F32,
            )
            scale = spec_flip[group, share, :].reshape(256, 128)
            waves = jnp.concatenate([waves[:, :128] * scale, waves[:, 128:] * scale], axis=1)
            back = jnp.dot(three_parts(waves), inverse[...], preferred_element_type=F32)
            column[group] = back.reshape(256 // ROWS, ROWS, 256)
            return inner

        lax.fori_loop(0, ROWS // 8, across, 0)

        def up(q, inner):
            rows = pl.ds(pl.multiple_of(q * 8, 8), 8)
            values = [(column[k, rows, 0:128], column[k, rows, 128:256]) for k in range(32)]
            values = short_transform(twisted(values, 1), 1)
            for s in range(32):
                staged[s, 0, rows, :] = values[s][0]
                staged[s, 1, rows, :] = values[s][1]
            return inner

        lax.fori_loop(0, ROWS // 8, up, 0)

        def pack(g, inner):
            for i in range(4):
                for part_at in range(2):
                    a, b = staged[4 * g + i, part_at, 0:8, :], staged[4 * g + i, part_at, 8:16, :]
                    send_b[chunk, 4 * g + i, 0, part_at] = jnp.where(left, a, pltpu.roll(b, 64, 1))
                    send_b[chunk, 4 * g + i, 1, part_at] = jnp.where(left, pltpu.roll(a, 64, 1), b)
            return inner

        lax.fori_loop(0, 8, pack, 0)

        send_back(chunk, 1)

        @pl.when(chunk < CLASSES - DEFERRED)
        def _():
            send_back(chunk, 0)

        return carry

    lax.fori_loop(0, CLASSES, columns, 0)

    def send_second(chunk, carry):
        send_back(chunk, 0)
        return carry

    lax.fori_loop(CLASSES - DEFERRED, CLASSES, send_second, 0)

    def inverse_half(chunk, half):
        halves = []
        for part_at in range(2):
            even = jnp.stack([recv_b[chunk, 2 * d, half, part_at] for d in range(16)])
            odd = jnp.stack([recv_b[chunk, 2 * d + 1, half, part_at] for d in range(16)])
            a, b = interlaced(even, odd)
            halves.append((a.reshape(128, 128).T, b.reshape(128, 128).T))
        both = jnp.concatenate(
            [jnp.concatenate([halves[0][i], halves[1][i]], axis=1) for i in range(2)], axis=0
        )
        result = jnp.dot(three_parts(both), inverse[...], preferred_element_type=F32)
        rows = pl.ds(64 * half, 64)
        for i in range(2):
            for k in range(2):
                at = chunk * SIZE + 2 * k + i
                cos, sin = twist[0, at, 0:1, :], twist[1, at, 0:1, :]
                first = 128 * i + 64 * k
                re, im = result[first : first + 64, :128], result[first : first + 64, 128:]
                work[at, rows, 0:128] = re * cos - im * sin
                work[at, rows, 128:256] = re * sin + im * cos

    def member_sum(b):
        rows = pl.ds(pl.multiple_of(b * 8, 8), 8)
        values = [
            (work[place_of(a), rows, 0:128], work[place_of(a), rows, 128:256]) for a in range(32)
        ]
        for a, (re, im) in enumerate(short_transform(values, 1)):
            lanes = slice(128 * a, 128 * a + 128)
            part[b, :, lanes] = held[0, rows, lanes] * re + held[1, rows, lanes] * im

    def to_core(t):
        return pltpu.make_async_remote_copy(
            src_ref=part.at[2 * t + 1 - core],
            dst_ref=recv_part.at[t],
            send_sem=part_sems.at[0, t],
            recv_sem=part_sems.at[1, t],
            device_id={"mem": other_core, "slab": me},
            device_id_type=MESH,
        )

    def to_chip(t):
        return pltpu.make_async_remote_copy(
            src_ref=pair.at[t],
            dst_ref=recv_pair.at[t],
            send_sem=pair_sems.at[0, t],
            recv_sem=pair_sems.at[1, t],
            device_id={"mem": other_chip, "slab": me},
            device_id_type=MESH,
        )

    def block_rows(block):
        return pl.ds(pl.multiple_of(block * 8, 8), 8)

    def finished(t):
        rows = block_rows(2 * t + core)
        return pltpu.make_async_remote_copy(
            src_ref=out.at[rows, :],
            dst_ref=out.at[rows, :],
            send_sem=total_sems.at[0, t],
            recv_sem=total_sems.at[1, t],
            device_id={"mem": other_core, "slab": me},
            device_id_type=MESH,
        )

    def pass_on(t):
        to_core(t).wait_recv()
        pair[t] = part[2 * t + core] + recv_part[t]
        to_chip(t).start()

    def sum_and_send(t, carry):
        member_sum(2 * t + 1 - core)
        to_core(t).start()
        member_sum(2 * t + core)

        @pl.when(t % 4 >= 1)
        def _():
            pass_on(t - 1)

        return carry

    for half in (1, 0):

        def last_rows(chunk, carry, half=half):
            arrived(send_b, recv_b, sems_b, 1, chunk, half)
            inverse_half(chunk, half)
            return carry

        lax.fori_loop(0, CLASSES, last_rows, 0)
        lax.fori_loop(4 * half, 4 * half + 4, sum_and_send, 0)
        pass_on(4 * half + 3)

    def finish(t, carry):
        to_chip(t).wait_recv()
        out[block_rows(2 * t + core), :] = pair[t] + recv_pair[t]
        finished(t).start()
        return carry

    lax.fori_loop(4, 8, finish, 0)
    lax.fori_loop(0, 4, finish, 0)

    def drain_slab(t, carry):
        for half in range(2):
            all_copies(send_a, recv_a, sems_a, t, half).wait_send()
            all_copies(send_b, recv_b, sems_b, t, half).wait_send()

        @pl.when(moved == 1)
        def _():
            own_copy(send_a, recv_a, 0, t).wait_send()
            own_copy(send_b, recv_b, 1, t).wait_send()

        return carry

    lax.fori_loop(0, CLASSES, drain_slab, 0)

    @pl.when(moved == 1)
    def _():
        for b in range(4):
            swap(b).wait_send()

    def drain(t, carry):
        to_core(t).wait_send()
        to_chip(t).wait_send()
        finished(t).wait_send()
        finished(t).wait_recv()
        return carry

    lax.fori_loop(0, 8, drain, 0)


def per_device(anomalies, increment, spectrum):
    tables, twist = constant_tables()
    vmem = pl.BlockSpec(memory_space=pltpu.VMEM)
    anywhere = pl.BlockSpec(memory_space=pl.ANY)
    dma = pltpu.SemaphoreType.DMA
    return pl.pallas_call(
        kernel,
        out_shape=pltpu.VMEM((128, 4096), F32),
        in_specs=[anywhere] * 7,
        out_specs=vmem,
        scratch_shapes=[
            pltpu.VMEM((256, 768), BF16),
            pltpu.VMEM((768, 256), BF16),
            pltpu.VMEM((768, 256), BF16),
            pltpu.VMEM((2, 32, 8, 128), F32),
            pltpu.VMEM((2, 128, 4096), BF16),
            pltpu.VMEM((2, 128, 4096), F32),
            pltpu.VMEM((2, 64, 4096), F32),
            pltpu.VMEM((128, 4096), F32),
            pltpu.VMEM((4096, 128), F32),
            pltpu.VMEM((128, 128), F32),
            pltpu.VMEM((32, 128, 128), F32),
            pltpu.VMEM((32, 128, 256), F32),
            pltpu.VMEM((CLASSES, 32, 2, 2, 8, 128), F32),
            pltpu.VMEM((CLASSES, 32, 2, 2, 8, 128), F32),
            pltpu.VMEM((32, ROWS, 256), F32),
            pltpu.VMEM((32, 2, ROWS, 128), F32),
            pltpu.VMEM((CLASSES, 32, 2, 2, 8, 128), F32),
            pltpu.VMEM((CLASSES, 32, 2, 2, 8, 128), F32),
            pltpu.VMEM((16, 8, 4096), F32),
            pltpu.VMEM((8, 8, 4096), F32),
            pltpu.VMEM((8, 8, 4096), F32),
            pltpu.VMEM((8, 8, 4096), F32),
            dma((21,)),
            dma((2, 4)),
            dma((2, 2, CLASSES)), dma((2, 2, CLASSES)), dma((2, 2, CLASSES)),
            dma((2, 8)), dma((2, 8)), dma((2, 8)),
        ],
        compiler_params=pltpu.CompilerParams(
            collective_id=0, has_side_effects=True, vmem_limit_bytes=58 * 2**20
        ),
        name="covariance",
    )(anomalies, increment, spectrum, *[jnp.asarray(t) for t in tables], jnp.asarray(twist))


def solution(mesh):
    placed = (P("mem", "slab", None), P("slab", None), P(None, "slab"))
    return jax.shard_map(
        per_device, mesh=mesh, in_specs=placed, out_specs=P("slab", None), check_vma=False
    )
```

```python
import math

import jax
import jax.numpy as jnp
import numpy as np
from jax import lax
from jax.experimental import pallas as pl
from jax.experimental.pallas import tpu as pltpu
from jax.sharding import PartitionSpec as P

MESH = pl.DeviceIdType.MESH
F32 = jnp.float32
BF16 = jnp.bfloat16
ROOT_HALF = math.sqrt(0.5)
CLASSES = 8
SIZE = 32 // CLASSES
HELD = 4
DEFERRED = 7
ROWS = 4 * SIZE

ROUNDS = (
    (2, 2), (1, 1), (3, 3), (0, 0), (1, 3), (3, 1), (0, 2), (2, 0),
    (1, 0), (3, 2), (1, 2), (3, 0), (0, 1), (2, 3), (2, 1), (0, 3),
)
OFFSETS = tuple(
    offset
    for a, b in ROUNDS
    for offset in ((a, b, 1), ((a + 2) % 4, (b + 2) % 4, 0))
    if offset != (0, 0, 0)
)


def constant_tables():
    index = np.arange(128)
    angle = 2.0 * np.pi / 128 * (np.outer(index, index) % 128)
    cos, sin = np.cos(angle), np.sin(angle)
    tables = []
    for sign in (-1.0, 1.0):
        block = np.block([[cos, sign * sin], [-sign * sin, cos]])
        if sign < 0:
            flipped = block.T
            high = flipped.astype(BF16)
            low = (flipped - high.astype(np.float64)).astype(BF16)
            tables.append(np.concatenate([high, high, low], axis=1))
        high = block.astype(BF16)
        low = (block - high.astype(np.float64)).astype(BF16)
        tables.append(np.concatenate([high, high, low], axis=0))
    order = np.arange(32) % SIZE * CLASSES + np.arange(32) // SIZE
    twist = 2.0 * np.pi / 4096 * np.outer(order, index)
    twist = np.stack([np.cos(twist), np.sin(twist)]).astype(np.float32)
    twist = np.broadcast_to(twist[:, :, None, :], (2, 32, 8, 128)).copy()
    return tables, twist


def short_transform(values, sign):
    count = len(values)
    if count == 1:
        return values
    even = short_transform(values[0::2], sign)
    odd = short_transform(values[1::2], sign)
    first, second = [], []
    for k in range(count // 2):
        (er, ei), (xr, xi) = even[k], odd[k]
        if k == 0:
            tr, ti = xr, xi
        elif 4 * k == count:
            if sign > 0:
                first.append((er - xi, ei + xr))
                second.append((er + xi, ei - xr))
            else:
                first.append((er + xi, ei - xr))
                second.append((er - xi, ei + xr))
            continue
        elif 8 * k == count:
            tr = (xr - sign * xi if sign > 0 else xr + xi) * ROOT_HALF
            ti = (xi + xr if sign > 0 else xi - xr) * ROOT_HALF
        elif 8 * k == 3 * count:
            tr = (xr + xi if sign > 0 else xr - xi) * -ROOT_HALF
            ti = (xr - xi if sign > 0 else -xr - xi) * ROOT_HALF
        else:
            cos = math.cos(2.0 * math.pi * k / count)
            sin = sign * math.sin(2.0 * math.pi * k / count)
            tr = xr * cos - xi * sin
            ti = xr * sin + xi * cos
        first.append((er + tr, ei + ti))
        second.append((er - tr, ei - ti))
    return first + second


def place_of(wave):
    return SIZE * (wave % CLASSES) + wave // CLASSES


def three_parts(x):
    high = x.astype(BF16)
    low = (x - high.astype(F32)).astype(BF16)
    return jnp.concatenate([high, low, high], axis=1)


def kernel(
    anomalies, increment, spectrum, flip_table, forward_table, inverse_table, twist_table, out,
    forward_flip, forward, inverse, twist,
    anom, held, given, incr, spec, turned, spec_flip, work, send_a, recv_a,
    column, staged, send_b, recv_b, part, recv_part, pair, recv_pair,
    load_sem, swap_sems, sems_a, sems_b, own_sems, part_sems, pair_sems, total_sems,
):
    me = lax.axis_index("slab")
    mem = lax.axis_index("mem")
    z, y, x = me // 8, (me // 2) % 4, me % 2
    core = mem % 2
    other_core = (mem // 2) * 2 + (1 - core)
    other_chip = (1 - mem // 2) * 2 + core
    moved = (x + core + 1) % 2

    def slab_at(offset):
        dz, dy, dx = offset
        return ((z + dz) % 4) * 8 + ((y + dy) % 4) * 2 + (x + dx) % 2

    barrier = pltpu.get_barrier_semaphore()
    for offset in OFFSETS:
        for mate in (mem, other_chip):
            pl.semaphore_signal(
                barrier,
                inc=1,
                device_id={"mem": mate, "slab": slab_at(offset)},
                device_id_type=MESH,
            )
    for mate in (other_core, other_chip):
        pl.semaphore_signal(
            barrier, inc=1, device_id={"mem": mate, "slab": me}, device_id_type=MESH
        )

    def load_anomalies(b):
        rows = pl.ds(pl.multiple_of(b * 16, 16), 16)
        return pltpu.make_async_copy(anomalies.at[:, rows, :], anom.at[:, rows, :], load_sem.at[b])

    def load_increment(b):
        rows = pl.ds(pl.multiple_of(b * 16, 16), 16)
        return pltpu.make_async_copy(increment.at[rows, :], incr.at[rows, :], load_sem.at[8 + b])

    def start_loads(b, carry):
        load_anomalies(b).start()
        load_increment(b).start()
        return carry

    load_twist = pltpu.make_async_copy(twist_table, twist, load_sem.at[17])
    load_flip = pltpu.make_async_copy(flip_table, forward_flip, load_sem.at[18])
    load_forward = pltpu.make_async_copy(forward_table, forward, load_sem.at[19])
    load_inverse = pltpu.make_async_copy(inverse_table, inverse, load_sem.at[20])
    load_spectrum = pltpu.make_async_copy(spectrum, spec, load_sem.at[16])
    lax.fori_loop(0, 8, start_loads, 0)
    for copy in (load_twist, load_flip, load_forward, load_inverse, load_spectrum):
        copy.start()

    sub = lax.broadcasted_iota(jnp.int32, (16, 8, 128), 1)
    lower = sub < 4
    left = lax.broadcasted_iota(jnp.int32, (8, 128), 1) < 64

    def interlaced(a, b):
        even = jnp.where(lower, a, pltpu.roll(b, 4, 1))
        odd = jnp.where(lower, pltpu.roll(a, 4, 1), b)
        return even, odd

    def twisted(values, sign):
        result = [values[0]]
        for k in range(1, 32):
            re, im = values[k]
            cos, sin = twist[0, place_of(k)], twist[1, place_of(k)]
            if sign > 0:
                result.append((re * cos - im * sin, re * sin + im * cos))
            else:
                result.append((re * cos + im * sin, im * cos - re * sin))
        return result

    def swap(b):
        rows = pl.ds(pl.multiple_of(b * 16, 16), 16)
        return pltpu.make_async_remote_copy(
            src_ref=given.at[:, rows, :],
            dst_ref=held.at[:, rows, :],
            send_sem=swap_sems.at[0, b],
            recv_sem=swap_sems.at[1, b],
            device_id={"mem": other_chip, "slab": me},
            device_id_type=MESH,
        )

    def widen(b, carry):
        load_anomalies(b).wait()
        load_increment(b).wait()
        rows = pl.ds(pl.multiple_of(b * 16, 16), 16)

        @pl.when((moved == 1) & (b < 4))
        def _():
            given[:, pl.ds(pl.multiple_of((b % 4) * 16, 16), 16), :] = anom[:, rows, :].astype(F32)

        @pl.when((moved == 0) | (b >= 4))
        def _():
            held[:, rows, :] = anom[:, rows, :].astype(F32)

        return carry

    def first_step(b, carry):
        rows = pl.ds(pl.multiple_of(b * 16, 16), 16)
        for n in range(SIZE):
            inputs = []
            for p in range(CLASSES):
                lanes = slice(128 * (n + SIZE * p), 128 * (n + SIZE * p) + 128)
                step = incr[rows, lanes]
                inputs.append(
                    (held[0, rows, lanes] * step, held[1, rows, lanes] * step)
                )
            for c, (re, im) in enumerate(short_transform(inputs, -1)):
                if c * n:
                    cos = math.cos(2.0 * math.pi * c * n / 32)
                    sin = -math.sin(2.0 * math.pi * c * n / 32)
                    re, im = re * cos - im * sin, re * sin + im * cos
                work[SIZE * c + n, rows, 0:128] = re
                work[SIZE * c + n, rows, 128:256] = im
        return carry

    lax.fori_loop(4, 8, widen, 0)
    lax.fori_loop(4, 8, first_step, 0)
    lax.fori_loop(0, 4, widen, 0)

    def mem_at(other):
        return ((mem // 2 + other) % 2) * 2 + core

    def half_copy(source, target, sems, chunk, half, slab, mate):
        return pltpu.make_async_remote_copy(
            src_ref=source.at[chunk, slab, half],
            dst_ref=target.at[chunk, me, half],
            send_sem=sems.at[0, half, chunk],
            recv_sem=sems.at[1, half, chunk],
            device_id={"mem": mate, "slab": slab},
            device_id_type=MESH,
        )

    def all_copies(source, target, sems, chunk, half):
        return pltpu.make_async_remote_copy(
            src_ref=source.at[chunk, 0:31, half],
            dst_ref=target.at[chunk, 0:31, half],
            send_sem=sems.at[0, half, chunk],
            recv_sem=sems.at[1, half, chunk],
            device_id={"mem": other_chip, "slab": me},
            device_id_type=MESH,
        )

    def own_copy(source, target, way, chunk):
        return pltpu.make_async_remote_copy(
            src_ref=source.at[chunk, me, 1],
            dst_ref=target.at[chunk, me, 1],
            send_sem=own_sems.at[way, 0, chunk],
            recv_sem=own_sems.at[way, 1, chunk],
            device_id={"mem": other_chip, "slab": me},
            device_id_type=MESH,
        )

    def keep_own(source, target, way, chunk, half):
        if half == 0:
            target[chunk, me, 0] = source[chunk, me, 0]
            return

        @pl.when(moved == 1)
        def _():
            own_copy(source, target, way, chunk).start()

        @pl.when(moved == 0)
        def _():
            target[chunk, me, 1] = source[chunk, me, 1]

    def arrived(source, target, sems, way, chunk, half):
        all_copies(source, target, sems, chunk, half).wait_recv()
        if half == 1:

            @pl.when(moved == 1)
            def _():
                own_copy(source, target, way, chunk).wait_recv()

    def send_forward(chunk, half):
        for offset in OFFSETS:
            mate = mem_at(offset[2] + moved * half)
            half_copy(send_a, recv_a, sems_a, chunk, half, slab_at(offset), mate).start()
        keep_own(send_a, recv_a, 0, chunk, half)

    def send_back(chunk, half):
        for offset in OFFSETS:
            mate = mem_at(offset[2] + ((moved + offset[2]) % 2) * half)
            half_copy(send_b, recv_b, sems_b, chunk, half, slab_at(offset), mate).start()
        keep_own(send_b, recv_b, 1, chunk, half)

    def forward_class(chunk, half):
        def second_step(b, inner):
            rows = pl.ds(pl.multiple_of(64 * half + b * 16, 16), 16)
            values = [
                (work[chunk * SIZE + n, rows, 0:128], work[chunk * SIZE + n, rows, 128:256])
                for n in range(SIZE)
            ]
            for m, (re, im) in enumerate(short_transform(values, -1)):
                at = chunk * SIZE + m
                cos, sin = twist[0, at, 0:1, :], twist[1, at, 0:1, :]
                work[at, rows, 0:128] = re * cos + im * sin
                work[at, rows, 128:256] = im * cos - re * sin
            return inner

        lax.fori_loop(0, 4, second_step, 0)
        rows = pl.ds(64 * half, 64)
        both = three_parts(
            jnp.concatenate([work[chunk * SIZE + m, rows, :] for m in (0, 2, 1, 3)], axis=0)
        )
        result = lax.dot_general(
            forward_flip[...], both, (((1,), (1,)), ((), ())), preferred_element_type=F32
        )
        for part_at in range(2):
            piece = result[128 * part_at : 128 * part_at + 128]
            even, odd = interlaced(
                piece[:, :128].reshape(16, 8, 128), piece[:, 128:].reshape(16, 8, 128)
            )
            for d in range(16):
                send_a[chunk, 2 * d, half, part_at] = even[d]
                send_a[chunk, 2 * d + 1, half, part_at] = odd[d]

    load_twist.wait()
    load_flip.wait()
    forward_class(0, 1)
    pl.semaphore_wait(barrier, 2 * len(OFFSETS) + 2)

    @pl.when(moved == 1)
    def _():
        for b in range(4):
            swap(b).start()

    send_forward(0, 1)

    def forward_second(chunk, carry):
        forward_class(chunk, 1)

        @pl.when((moved == 0) | (chunk < HELD))
        def _():
            send_forward(chunk, 1)

        return carry

    lax.fori_loop(1, CLASSES, forward_second, 0)

    load_forward.wait()
    load_inverse.wait()
    load_spectrum.wait()

    def flip_spectrum(k, carry):
        piece = spec[pl.ds(k, 128, stride=32), :] * (1.0 / (4096.0 * 4096.0))
        turned[...] = piece.T
        for c in range(CLASSES):
            for b in range(4):
                spec_flip[k, pl.ds(ROWS * c + b, SIZE, stride=4), :] = turned[
                    pl.ds(32 * b + c, SIZE, stride=CLASSES), :
                ]
        return carry

    lax.fori_loop(0, 32, flip_spectrum, 0)

    def late_step(b, carry):
        @pl.when(moved == 1)
        def _():
            swap(b).wait_recv()

        return first_step(b, carry)

    lax.fori_loop(0, 4, late_step, 0)

    def forward_first(chunk, carry):
        @pl.when((moved == 1) & (chunk >= HELD))
        def _():
            send_forward(chunk, 1)

        forward_class(chunk, 0)
        send_forward(chunk, 0)
        return carry

    lax.fori_loop(0, CLASSES, forward_first, 0)

    def columns(chunk, carry):
        arrived(send_a, recv_a, sems_a, 0, chunk, 1)
        arrived(send_a, recv_a, sems_a, 0, chunk, 0)

        def unpack(g, inner):
            for i in range(4):
                for part_at in range(2):
                    a = recv_a[chunk, 4 * g + i, 0, part_at]
                    b = recv_a[chunk, 4 * g + i, 1, part_at]
                    staged[4 * g + i, part_at, 0:8, :] = jnp.where(left, a, pltpu.roll(b, 64, 1))
                    staged[4 * g + i, part_at, 8:16, :] = jnp.where(left, pltpu.roll(a, 64, 1), b)
            return inner

        lax.fori_loop(0, 8, unpack, 0)

        def down(q, inner):
            rows = pl.ds(pl.multiple_of(q * 8, 8), 8)
            values = [
                (staged[s, 0, rows, :], staged[s, 1, rows, :]) for s in range(32)
            ]
            values = twisted(short_transform(values, -1), -1)
            for k in range(32):
                column[k, rows, 0:128] = values[k][0]
                column[k, rows, 128:256] = values[k][1]
            return inner

        lax.fori_loop(0, ROWS // 8, down, 0)
        share = pl.ds(pl.multiple_of(chunk * ROWS, ROWS), ROWS)

        def across(g, inner):
            group = pl.ds(pl.multiple_of(g * 256 // ROWS, 256 // ROWS), 256 // ROWS)
            waves = jnp.dot(
                three_parts(column[group].reshape(256, 256)), forward[...],
                preferred_element_type=F32,
            )
            scale = spec_flip[group, share, :].reshape(256, 128)
            waves = jnp.concatenate([waves[:, :128] * scale, waves[:, 128:] * scale], axis=1)
            back = jnp.dot(three_parts(waves), inverse[...], preferred_element_type=F32)
            column[group] = back.reshape(256 // ROWS, ROWS, 256)
            return inner

        lax.fori_loop(0, ROWS // 8, across, 0)

        def up(q, inner):
            rows = pl.ds(pl.multiple_of(q * 8, 8), 8)
            values = [(column[k, rows, 0:128], column[k, rows, 128:256]) for k in range(32)]
            values = short_transform(twisted(values, 1), 1)
            for s in range(32):
                staged[s, 0, rows, :] = values[s][0]
                staged[s, 1, rows, :] = values[s][1]
            return inner

        lax.fori_loop(0, ROWS // 8, up, 0)

        def pack(g, inner):
            for i in range(4):
                for part_at in range(2):
                    a, b = staged[4 * g + i, part_at, 0:8, :], staged[4 * g + i, part_at, 8:16, :]
                    send_b[chunk, 4 * g + i, 0, part_at] = jnp.where(left, a, pltpu.roll(b, 64, 1))
                    send_b[chunk, 4 * g + i, 1, part_at] = jnp.where(left, pltpu.roll(a, 64, 1), b)
            return inner

        lax.fori_loop(0, 8, pack, 0)

        send_back(chunk, 1)

        @pl.when(chunk < CLASSES - DEFERRED)
        def _():
            send_back(chunk, 0)

        return carry

    lax.fori_loop(0, CLASSES, columns, 0)

    def send_second(chunk, carry):
        send_back(chunk, 0)
        return carry

    lax.fori_loop(CLASSES - DEFERRED, CLASSES, send_second, 0)

    def inverse_half(chunk, half):
        halves = []
        for part_at in range(2):
            even = jnp.stack([recv_b[chunk, 2 * d, half, part_at] for d in range(16)])
            odd = jnp.stack([recv_b[chunk, 2 * d + 1, half, part_at] for d in range(16)])
            a, b = interlaced(even, odd)
            halves.append((a.reshape(128, 128).T, b.reshape(128, 128).T))
        both = jnp.concatenate(
            [jnp.concatenate([halves[0][i], halves[1][i]], axis=1) for i in range(2)], axis=0
        )
        result = jnp.dot(three_parts(both), inverse[...], preferred_element_type=F32)
        rows = pl.ds(64 * half, 64)
        for i in range(2):
            for k in range(2):
                at = chunk * SIZE + 2 * k + i
                cos, sin = twist[0, at, 0:1, :], twist[1, at, 0:1, :]
                first = 128 * i + 64 * k
                re, im = result[first : first + 64, :128], result[first : first + 64, 128:]
                work[at, rows, 0:128] = re * cos - im * sin
                work[at, rows, 128:256] = re * sin + im * cos

    def member_sum(b):
        rows = pl.ds(pl.multiple_of(b * 8, 8), 8)
        values = [
            (work[place_of(a), rows, 0:128], work[place_of(a), rows, 128:256]) for a in range(32)
        ]
        for a, (re, im) in enumerate(short_transform(values, 1)):
            lanes = slice(128 * a, 128 * a + 128)
            part[b, :, lanes] = held[0, rows, lanes] * re + held[1, rows, lanes] * im

    def to_core(t):
        return pltpu.make_async_remote_copy(
            src_ref=part.at[2 * t + 1 - core],
            dst_ref=recv_part.at[t],
            send_sem=part_sems.at[0, t],
            recv_sem=part_sems.at[1, t],
            device_id={"mem": other_core, "slab": me},
            device_id_type=MESH,
        )

    def to_chip(t):
        return pltpu.make_async_remote_copy(
            src_ref=pair.at[t],
            dst_ref=recv_pair.at[t],
            send_sem=pair_sems.at[0, t],
            recv_sem=pair_sems.at[1, t],
            device_id={"mem": other_chip, "slab": me},
            device_id_type=MESH,
        )

    def block_rows(block):
        return pl.ds(pl.multiple_of(block * 8, 8), 8)

    def finished(t):
        rows = block_rows(2 * t + core)
        return pltpu.make_async_remote_copy(
            src_ref=out.at[rows, :],
            dst_ref=out.at[rows, :],
            send_sem=total_sems.at[0, t],
            recv_sem=total_sems.at[1, t],
            device_id={"mem": other_core, "slab": me},
            device_id_type=MESH,
        )

    def pass_on(t):
        to_core(t).wait_recv()
        pair[t] = part[2 * t + core] + recv_part[t]
        to_chip(t).start()

    def sum_and_send(t, carry):
        member_sum(2 * t + 1 - core)
        to_core(t).start()
        member_sum(2 * t + core)

        @pl.when(t % 4 >= 1)
        def _():
            pass_on(t - 1)

        return carry

    for half in (1, 0):

        def last_rows(chunk, carry, half=half):
            arrived(send_b, recv_b, sems_b, 1, chunk, half)
            inverse_half(chunk, half)
            return carry

        lax.fori_loop(0, CLASSES, last_rows, 0)
        lax.fori_loop(4 * half, 4 * half + 4, sum_and_send, 0)
        pass_on(4 * half + 3)

    def finish(t, carry):
        to_chip(t).wait_recv()
        out[block_rows(2 * t + core), :] = pair[t] + recv_pair[t]
        finished(t).start()
        return carry

    lax.fori_loop(4, 8, finish, 0)
    lax.fori_loop(0, 4, finish, 0)

    def drain_slab(t, carry):
        for half in range(2):
            all_copies(send_a, recv_a, sems_a, t, half).wait_send()
            all_copies(send_b, recv_b, sems_b, t, half).wait_send()

        @pl.when(moved == 1)
        def _():
            own_copy(send_a, recv_a, 0, t).wait_send()
            own_copy(send_b, recv_b, 1, t).wait_send()

        return carry

    lax.fori_loop(0, CLASSES, drain_slab, 0)

    @pl.when(moved == 1)
    def _():
        for b in range(4):
            swap(b).wait_send()

    def drain(t, carry):
        to_core(t).wait_send()
        to_chip(t).wait_send()
        finished(t).wait_send()
        finished(t).wait_recv()
        return carry

    lax.fori_loop(0, 8, drain, 0)


def per_device(anomalies, increment, spectrum):
    tables, twist = constant_tables()
    vmem = pl.BlockSpec(memory_space=pltpu.VMEM)
    anywhere = pl.BlockSpec(memory_space=pl.ANY)
    dma = pltpu.SemaphoreType.DMA
    return pl.pallas_call(
        kernel,
        out_shape=pltpu.VMEM((128, 4096), F32),
        in_specs=[anywhere] * 7,
        out_specs=vmem,
        scratch_shapes=[
            pltpu.VMEM((256, 768), BF16),
            pltpu.VMEM((768, 256), BF16),
            pltpu.VMEM((768, 256), BF16),
            pltpu.VMEM((2, 32, 8, 128), F32),
            pltpu.VMEM((2, 128, 4096), BF16),
            pltpu.VMEM((2, 128, 4096), F32),
            pltpu.VMEM((2, 64, 4096), F32),
            pltpu.VMEM((128, 4096), F32),
            pltpu.VMEM((4096, 128), F32),
            pltpu.VMEM((128, 128), F32),
            pltpu.VMEM((32, 128, 128), F32),
            pltpu.VMEM((32, 128, 256), F32),
            pltpu.VMEM((CLASSES, 32, 2, 2, 8, 128), F32),
            pltpu.VMEM((CLASSES, 32, 2, 2, 8, 128), F32),
            pltpu.VMEM((32, ROWS, 256), F32),
            pltpu.VMEM((32, 2, ROWS, 128), F32),
            pltpu.VMEM((CLASSES, 32, 2, 2, 8, 128), F32),
            pltpu.VMEM((CLASSES, 32, 2, 2, 8, 128), F32),
            pltpu.VMEM((16, 8, 4096), F32),
            pltpu.VMEM((8, 8, 4096), F32),
            pltpu.VMEM((8, 8, 4096), F32),
            pltpu.VMEM((8, 8, 4096), F32),
            dma((21,)),
            dma((2, 4)),
            dma((2, 2, CLASSES)), dma((2, 2, CLASSES)), dma((2, 2, CLASSES)),
            dma((2, 8)), dma((2, 8)), dma((2, 8)),
        ],
        compiler_params=pltpu.CompilerParams(
            collective_id=0, has_side_effects=True, vmem_limit_bytes=58 * 2**20
        ),
        name="covariance",
    )(anomalies, increment, spectrum, *[jnp.asarray(t) for t in tables], jnp.asarray(twist))


def solution(mesh):
    placed = (P("mem", "slab", None), P("slab", None), P(None, "slab"))
    return jax.shard_map(
        per_device, mesh=mesh, in_specs=placed, out_specs=P("slab", None), check_vma=False
    )
```
